32 devices in a mesh: groups: 2 (over y), rows: 4 (over z), cols: 2 (over x), sub: 2 (over core).
Axes of the slice: x: 2, y: 2, z: 4, core: 2. Of those that a mesh axis runs over, the one named last changes fastest.
Arguments:
- diagonal_tiles: float32 [256, 128, 128], P(('groups', 'rows', 'sub')), parts along dimension 0
- coupling_tiles: float32 [256, 6, 128, 128], P(('groups', 'rows', 'sub'), 'cols'), parts along dimension 0, may hold values from -0.0625 to 0.0625
- column_part: int32 [256, 6], P(('groups', 'rows', 'sub'), 'cols'), parts along dimension 0, may hold values from 0 to 4
- column_tile: int32 [256, 6], P(('groups', 'rows', 'sub'), 'cols'), parts along dimension 0, may hold values from 0 to 31
- neighbours: int32 [8, 4], P('groups'), parts along dimension 0, may hold values from 0 to 3, as said below
- right_side: float32 [256, 128], P(('groups', 'rows', 'sub')), parts along dimension 0, may hold values from -6 to 6
- jacobi_inverse: float32 [256, 128, 128], P(('groups', 'rows', 'sub')), parts along dimension 0, as said below
Outputs:
- solution: float32 [256, 128], P(('groups', 'rows', 'sub')), parts along dimension 0
- residual: float32 [256, 128], P(('groups', 'rows', 'sub')), parts along dimension 0
The draws below stay inside these ranges and needn't reach their ends.
There are 2 independent parts, one for each index of `groups`. The reference program is written for one: setup_inputs(seed, part) draws one part's arguments, and reference() takes and returns one part's arrays. A program takes and returns all parts, laid end to end along the dimension named above; each array names one. Nothing has to cross between parts.
Inputs may be any that keep to these rules, and one draw needn't show every extreme that they name: `neighbours`: entry 0 of partition p's list is (p + 4 // 2) mod 4, the opposite partition on the cycle; every other entry names a partition whose index differs from p by 1 to 2 (without wrapping round); entries may repeat. `jacobi_inverse`: block-diagonal: each group of 5 consecutive variables, from the first on, forms one 5 x 5 block, and each variable left over after the last whole group of 5 is a 1 x 1 block of its own.
All inputs are finite; a program needn't handle non-finite values.
Results may differ from the reference program's by a relative error of at most 0.00019.
Values sent between devices are 32-bit elements; how exact they have to be, the bound alone decides.
A program may use at most 64 MiB of HBM per device.

```python
import jax
import jax.numpy as jnp
from jax import lax

TW = 128
NR = 2
ITERS = 2
RB = 32
NB = 128
K = 6
NNB = 4
N_ROWS = 4


def draw_diagonal_tiles(key, part):
    first, second = jax.random.split(jax.random.fold_in(key, 11))
    scales = jax.random.uniform(first, (NB, TW, 1), jnp.float32, 1.5, 2.5)
    noise = jax.random.normal(second, (NB, TW, TW), jnp.float32)
    return scales * jnp.eye(TW, dtype=jnp.float32) + 0.3 / TW ** 0.5 * noise


def draw_jacobi_inverse(key, part):
    first, second = jax.random.split(jax.random.fold_in(key, 23))
    index = jnp.arange(TW, dtype=jnp.int32)
    cutoff = TW // 5 * 5
    blocks = jnp.where(index < cutoff, index // 5, TW + index)
    inside = (blocks[:, None] == blocks[None, :]).astype(jnp.float32)
    scales = jax.random.uniform(first, (NB, TW, 1), jnp.float32, 0.4, 1.0)
    noise = jax.random.normal(second, (NB, TW, TW), jnp.float32) * 0.15
    return (scales * jnp.eye(TW, dtype=jnp.float32) + noise) * inside


def draw_neighbours(key, part):
    picked = jax.random.randint(jax.random.fold_in(key, 37), (N_ROWS, NNB), 0, NNB)
    offset = jnp.where(picked < NR, picked - NR, picked - NR + 1)
    owner = jnp.arange(N_ROWS, dtype=jnp.int32)[:, None]
    target = owner + offset
    target = jnp.where((target < 0) | (target >= N_ROWS), owner - offset, target)
    opposite = (owner + N_ROWS // 2) % N_ROWS
    column = jnp.arange(NNB, dtype=jnp.int32)[None, :]
    target = jnp.where(column == 0, opposite, target)
    return target.astype(jnp.int32)


def set_ends(entries, key, smallest, largest):
    dims = entries.shape
    index_at = [jax.random.randint(jax.random.fold_in(key, axis), (), 0, dims[axis]) for axis in range(len(dims))]
    entries = entries.at[tuple(index_at)].set(smallest)
    longest = dims.index(max(dims))
    index_at[longest] = (index_at[longest] + 1) % dims[longest]
    return entries.at[tuple(index_at)].set(largest)


def level_of(key, dims, shards, least, largest):
    level = 1.0
    for axis_at, parts in shards:
        steps = jax.random.uniform(jax.random.fold_in(jax.random.fold_in(key, 6), axis_at), (parts,), jnp.float32, least / len(shards), largest / len(shards))
        level = level * jnp.repeat(jnp.exp(steps), dims[axis_at] // parts).reshape((-1,) + (1,) * (len(dims) - 1 - axis_at))
    return level


def gaussian(own_key, extent, deviation, limit, cuts=(), kind=jnp.bfloat16):
    result = deviation * jax.random.normal(own_key, extent, jnp.float32)
    if cuts:
        result = result * level_of(own_key, extent, cuts, -0.22, 0.18)
    return jnp.clip(result, -limit, limit).astype(kind)


def setup_inputs(seed: int = 0, part: int = 0) -> dict:
    splits = jax.random.split(jax.random.key(seed), 8)
    part_splits = jax.random.split(jax.random.fold_in(splits[7], part), 8)
    diagonal_tiles = draw_diagonal_tiles(jax.random.fold_in(jax.random.fold_in(splits[7], part), 71), part)
    coupling_tiles = gaussian(part_splits[1], (NB, K, TW, TW), (11 * K * TW) ** -0.5, 0.0625, ((0, 8), (1, 2)), jnp.float32)
    column_part = set_ends(jax.random.randint(part_splits[2], (NB, K), 0, NNB + 1), jax.random.fold_in(part_splits[2], 1), 0, NNB).astype(jnp.int32)
    column_tile = set_ends(jax.random.randint(part_splits[3], (NB, K), 0, RB), jax.random.fold_in(part_splits[3], 1), 0, RB - 1).astype(jnp.int32)
    neighbours = draw_neighbours(jax.random.fold_in(jax.random.fold_in(splits[7], part), 71), part)
    right_side = gaussian(part_splits[5], (NB, TW), 1.0, 6.0, ((0, 8),), jnp.float32)
    jacobi_inverse = draw_jacobi_inverse(jax.random.fold_in(jax.random.fold_in(splits[7], part), 71), part)
    return dict(diagonal_tiles=diagonal_tiles, coupling_tiles=coupling_tiles, column_part=column_part, column_tile=column_tile, neighbours=neighbours, right_side=right_side, jacobi_inverse=jacobi_inverse)


def transpose_apply(vector, diagonal_tiles, coupling_tiles, column_part, column_tile, neighbours):
    highest = lax.Precision.HIGHEST
    diagonal_part = jnp.einsum('rij,ri->rj', diagonal_tiles, vector, precision=highest)
    partial_value = jnp.einsum('rkij,ri->rkj', coupling_tiles, vector, precision=highest)
    tile_rows = vector.shape[0]
    part_rows = tile_rows // N_ROWS
    owner = jnp.arange(tile_rows, dtype=jnp.int32) // part_rows
    listed = neighbours[owner]
    chosen = jnp.take_along_axis(listed, jnp.maximum(column_part - 1, 0).astype(jnp.int32), axis=1)
    target = jnp.where(column_part == 0, owner[:, None], chosen)
    landing = (target * part_rows + column_tile).astype(jnp.int32).reshape(-1)
    summed = jax.ops.segment_sum(partial_value.reshape(-1, partial_value.shape[-1]), landing, num_segments=tile_rows)
    return diagonal_part + summed


def precondition(jacobi_inverse, vector):
    return jnp.einsum('rij,ri->rj', jacobi_inverse, vector, precision=lax.Precision.HIGHEST)


def reference(diagonal_tiles, coupling_tiles, column_part, column_tile, neighbours, right_side, jacobi_inverse):
    def apply_a(vector):
        return transpose_apply(vector, diagonal_tiles, coupling_tiles, column_part, column_tile, neighbours)

    solution = jnp.zeros_like(right_side)
    residual = right_side
    shadow = right_side
    search = right_side
    rho_now = jnp.sum(shadow * residual)
    for step in range(ITERS):
        search_hat = precondition(jacobi_inverse, search)
        image = apply_a(search_hat)
        alpha = rho_now / jnp.sum(shadow * image)
        half = residual - alpha * image
        half_hat = precondition(jacobi_inverse, half)
        twice = apply_a(half_hat)
        omega = jnp.sum(twice * half) / jnp.sum(twice * twice)
        solution = solution + alpha * search_hat + omega * half_hat
        residual = half - omega * twice
        if step + 1 < ITERS:
            rho_next = jnp.sum(shadow * residual)
            search = residual + (rho_next / rho_now) * (alpha / omega) * (search - omega * image)
            rho_now = rho_next
    return solution, residual
```

```python
import functools

import jax
import jax.numpy as jnp
from jax import lax
from jax.experimental import pallas as pl
from jax.experimental.pallas import tpu as pltpu
from jax.sharding import PartitionSpec as P

MESH = pl.DeviceIdType.MESH
REACH = 2
APPLIES = 4
SUBLANES = 8
MOST_DOTS = 4
F32 = jnp.float32


def offsets_of(count):
    wanted = {d % count for d in range(-REACH, REACH + 1)} | {count // 2}
    return sorted(wanted)


def pieces_of(rows):
    return 8 if rows % 8 == 0 else 1


def kernel(
    sizes,
    diag_hbm,
    coup_hbm,
    jac_hbm,
    part_hbm,
    tile_hbm,
    near_hbm,
    right_hbm,
    out_ref,
    diag,
    coup,
    jac,
    part_ref,
    tile_ref,
    near_ref,
    right_ref,
    one_hot,
    prod,
    dprod,
    vec,
    landed,
    recv,
    dots,
    dots_recv,
    load_sem,
    send_sem,
    recv_sem,
    dots_send_sem,
    dots_recv_sem,
):
    n_rows, n_cols, n_sub = sizes
    offsets = offsets_of(n_rows)
    slots = len(offsets)
    rows_dev, slot_count, width, _ = coup.shape
    half_rows = slots * rows_dev
    chunk = rows_dev * SUBLANES
    peers = n_rows * n_sub
    unroll = pieces_of(rows_dev)
    row = lax.axis_index("rows")
    col = lax.axis_index("cols")
    sub = lax.axis_index("sub")
    me = row * n_sub + sub

    def piece_loads(g):
        at = pl.ds(g * unroll, unroll)
        return [
            pltpu.make_async_copy(diag_hbm.at[at], diag.at[at], load_sem.at[5 + 2 * g]),
            pltpu.make_async_copy(coup_hbm.at[at], coup.at[at], load_sem.at[6 + 2 * g]),
        ]

    small = [
        pltpu.make_async_copy(part_hbm, part_ref, load_sem.at[0]),
        pltpu.make_async_copy(tile_hbm, tile_ref, load_sem.at[1]),
        pltpu.make_async_copy(near_hbm, near_ref, load_sem.at[2]),
        pltpu.make_async_copy(right_hbm, right_ref, load_sem.at[3]),
    ]
    jac_load = pltpu.make_async_copy(jac_hbm, jac, load_sem.at[4])
    for load in small:
        load.start()
    jac_load.start()
    for g in range(rows_dev // unroll):
        for load in piece_loads(g):
            load.start()

    def partner(slot):
        return lax.rem(row + offsets[slot], n_rows)

    def always(slot):
        return offsets[slot] in (0, n_rows // 2)

    def is_linked(slot):
        return jnp.abs(partner(slot) - row) <= REACH

    def if_linked(slot, act):
        if always(slot):
            act()
        else:
            pl.when(is_linked(slot))(act)

    maybe = [slot for slot in range(slots) if not always(slot)]
    linked_count = slots - len(maybe)
    for slot in maybe:
        linked_count = linked_count + is_linked(slot).astype(jnp.int32)

    def for_linked_count(act):
        if not maybe:
            act(slots)
        for total in range(slots - len(maybe), slots + 1) if maybe else ():
            pl.when(linked_count == total)(functools.partial(act, total))

    def corner(slot, step):
        return {
            "rows": partner(slot),
            "cols": lax.rem(col + step // n_sub, n_cols),
            "sub": lax.rem(sub + step % n_sub, n_sub),
        }

    barrier = pltpu.get_barrier_semaphore()

    def dot_peers():
        for step in range(1, peers):
            peer = lax.rem(me + step, peers)
            yield peer, {"rows": lax.div(peer, n_sub), "cols": col, "sub": lax.rem(peer, n_sub)}

    def from_block(slot, c, s):
        return ((slot * n_cols + c) * n_sub + s) * rows_dev

    per_slot = n_cols * n_sub * rows_dev
    for slot in maybe:
        at = pl.ds(slot * per_slot, per_slot)
        for e in range(APPLIES):
            recv[e, at] = jnp.zeros((per_slot, width), F32)

    far_first = sorted(range(slots), key=lambda s: -min(offsets[s], n_rows - offsets[s]))
    for slot in far_first:
        for step in range(n_sub, n_cols * n_sub):

            def greet(slot=slot, step=step):
                where = corner(slot, step)
                pl.semaphore_signal(barrier, inc=1, device_id=where, device_id_type=MESH)

            if_linked(slot, greet)
    for _, where in dot_peers():
        pl.semaphore_signal(barrier, inc=1, device_id=where, device_id_type=MESH)

    for load in small:
        load.wait()
    part = part_ref[...]
    tile = tile_ref[...]
    target = jnp.full(part.shape, row, jnp.int32)
    for j in range(near_ref.shape[1]):
        target = jnp.where(part == j + 1, near_ref[row, j], target)
    apart = target - row
    apart = jnp.where(apart < 0, apart + n_rows, apart)
    place = jnp.zeros(part.shape, jnp.int32)
    for slot in range(1, slots):
        place = jnp.where(apart == offsets[slot], slot, place)
    landing = place * rows_dev + tile
    for j in range(1, n_sub):
        landing = jnp.where(tile >= j * rows_dev, landing + (half_rows - rows_dev), landing)
    from_row = lax.broadcasted_iota(jnp.int32, (rows_dev, chunk), 0)
    to_lane = lax.broadcasted_iota(jnp.int32, (rows_dev, chunk), 1)
    first = from_row * SUBLANES
    spread = ((to_lane >= first) & (to_lane < first + SUBLANES)).astype(F32)
    spread_landing = jnp.dot(
        landing.astype(F32), spread, precision=lax.Precision.HIGHEST, preferred_element_type=F32
    )
    at_row = lax.broadcasted_iota(jnp.int32, (n_sub * half_rows, chunk), 0).astype(F32)
    for k in range(slot_count):
        hit = (spread_landing[k : k + 1] == at_row).astype(F32)
        one_hot[:, k * chunk : (k + 1) * chunk] = hit.astype(jnp.bfloat16)

    jac_load.wait()

    def turn(r, carry):
        jac[r] = jnp.transpose(jac[r])
        return carry

    lax.fori_loop(0, rows_dev, turn, 0, unroll=4)

    def owner_copy(e, slot, step):
        back = offsets.index(-offsets[slot] % n_rows)
        where = corner(slot, step)
        at = pl.multiple_of(where["sub"] * half_rows + slot * rows_dev, rows_dev)
        to = pl.multiple_of(from_block(back, col, sub), rows_dev)
        return pltpu.make_async_remote_copy(
            src_ref=landed.at[e, pl.ds(at, rows_dev)],
            dst_ref=recv.at[e, pl.ds(to, rows_dev)],
            send_sem=send_sem.at[e],
            recv_sem=recv_sem.at[e],
            device_id=where,
            device_id_type=MESH,
        )

    routes = [(s, c) for s in far_first for c in reversed(range(n_cols * n_sub)) if (s, c) != (0, 0)]

    def each_route(act):
        for slot, step in routes:
            if_linked(slot, functools.partial(act, slot, step))

    def await_rows(sem, count):
        some = recv.at[0, pl.ds(0, count)]
        pltpu.make_async_copy(some, some, sem).wait()

    def await_blocks(sem):
        for_linked_count(lambda total: await_rows(sem, total * per_slot - rows_dev))

    def dots_copy(e, count, where):
        return pltpu.make_async_remote_copy(
            src_ref=dots.at[e, pl.ds(0, count)],
            dst_ref=dots_recv.at[e, me, pl.ds(0, count)],
            send_sem=dots_send_sem.at[e],
            recv_sem=dots_recv_sem.at[e],
            device_id=where,
            device_id_type=MESH,
        )

    def dots_start(e, products):
        count = len(products)
        lines = [jnp.sum(product, axis=0, keepdims=True) for product in products]
        for j, line in enumerate(lines):
            dots[e, j : j + 1] = line
        for _, where in dot_peers():
            dots_copy(e, count, where).start()
        for j, line in enumerate(lines):
            dots_recv[e, me, j : j + 1] = line

    def dots_finish(e, count):
        await_rows(dots_recv_sem.at[e], (peers - 1) * count)
        lines = jnp.sum(dots_recv[e, :, :count], axis=0)
        total = jnp.sum(lines, axis=1, keepdims=True)
        return [jnp.broadcast_to(total[j : j + 1], (1, width)) for j in range(count)]

    def fold(product):
        return jnp.sum(product.reshape(width // SUBLANES, SUBLANES, width), axis=0)

    def send_products(e, value):
        if e > 0:
            vec[e] = value

        def some_rows(g, carry):
            if e == 0:
                for load in piece_loads(g):
                    load.wait()
            for u in range(unroll):
                r = g * unroll + u
                line = vec[e, pl.ds(r, 1)] if e > 0 else right_ref[pl.ds(r, 1)]
                hat = jnp.sum(jac[r] * line, axis=1, keepdims=True)
                hat = jnp.broadcast_to(hat, (width, width))
                for k in range(slot_count):
                    at = pl.multiple_of(k * chunk + r * SUBLANES, SUBLANES)
                    prod[pl.ds(at, SUBLANES)] = fold(coup[r, k] * hat)
                dprod[pl.ds(pl.multiple_of(r * SUBLANES, SUBLANES), SUBLANES)] = fold(diag[r] * hat)
            return carry

        lax.fori_loop(0, rows_dev // unroll, some_rows, 0)
        rest = prod[...]
        out = None
        for _ in range(3):
            piece = rest.astype(jnp.bfloat16)
            rest = rest - piece.astype(F32)
            term = jnp.dot(one_hot[...], piece, preferred_element_type=F32)
            out = term if out is None else out + term
        landed[e] = out
        if e == 0:
            greetings = peers - 1 + (n_cols - 1) * n_sub * linked_count
            pl.semaphore_wait(barrier, greetings)
        each_route(lambda slot, step: owner_copy(e, slot, step).start())

    def own_products(e):
        at = pl.multiple_of(from_block(0, col, sub), rows_dev)
        from_at = pl.multiple_of(sub * half_rows, rows_dev)
        recv[e, pl.ds(at, rows_dev)] = landed[e, pl.ds(from_at, rows_dev)]
        return jnp.sum(dprod[...].reshape(rows_dev, SUBLANES, width), axis=1)

    def gather_products(e, own):
        await_blocks(recv_sem.at[e])
        for b in range(slots * n_cols * n_sub):
            own = own + recv[e, b * rows_dev : (b + 1) * rows_dev]
        return own

    shadow = right_ref[...]
    send_products(0, shadow)
    own = own_products(0)
    image = gather_products(0, own)

    send_products(1, image)
    dots_start(0, [shadow * shadow, shadow * image])
    own = own_products(1)
    rho, shadow_image = dots_finish(0, 2)
    alpha = rho / shadow_image
    half = shadow - alpha * image
    second = gather_products(1, own)
    twice = image - alpha * second

    send_products(2, twice)
    dots_start(1, [twice * half, twice * twice, shadow * half, shadow * twice])
    own = own_products(2)
    cross, square, shadow_half, shadow_twice = dots_finish(1, 4)
    omega = cross / square
    rho_next = shadow_half - omega * shadow_twice
    beta = rho_next / rho * (alpha / omega)
    residual = half - omega * twice
    search = residual + beta * (shadow - omega * image)
    known = twice + beta * (image - omega * second)
    third = gather_products(2, own)
    residual_image = twice - omega * third
    image = known - omega * third

    send_products(3, image)
    dots_start(2, [shadow * image])
    own = own_products(3)
    alpha_next = rho_next / dots_finish(2, 1)[0]
    half_next = residual - alpha_next * image
    fourth = gather_products(3, own)
    twice = residual_image - alpha_next * fourth
    dots_start(3, [twice * half_next, twice * twice])

    vec[0] = alpha * shadow + omega * half + alpha_next * search
    vec[1] = half_next
    at_lane = lax.broadcasted_iota(jnp.int32, (width, width), 1)

    def hats(r, carry):
        for j in range(2):
            hat = jnp.sum(jac[r] * vec[j, pl.ds(r, 1)], axis=1, keepdims=True)
            carry = jnp.where(at_lane == j * rows_dev + r, hat, carry)
        return carry

    hat = lax.fori_loop(0, rows_dev, hats, jnp.zeros((width, width), F32), unroll=4)
    hat = jnp.transpose(hat)
    for e in range(APPLIES):
        await_blocks(send_sem.at[e])
    cross, square = dots_finish(3, 2)
    omega = cross / square
    out_ref[:rows_dev] = hat[:rows_dev] + omega * hat[rows_dev : 2 * rows_dev]
    out_ref[rows_dev:] = half_next - omega * twice
    for e, count in enumerate((2, 4, 1, 2)):
        await_rows(dots_send_sem.at[e], (peers - 1) * count)


def on_device(
    diagonal_tiles, coupling_tiles, column_part, column_tile, neighbours, right_side, jacobi_inverse
):
    n_rows, n_cols, n_sub = (lax.axis_size(a) for a in ("rows", "cols", "sub"))
    slots = len(offsets_of(n_rows))
    rows_dev, slot_count, width, _ = coupling_tiles.shape
    half_rows = slots * rows_dev
    chunk = rows_dev * SUBLANES
    peers = n_rows * n_sub
    hbm = pl.BlockSpec(memory_space=pl.ANY)
    vmem = pl.BlockSpec(memory_space=pltpu.VMEM)
    dma = pltpu.SemaphoreType.DMA
    scratch = [
        pltpu.VMEM(diagonal_tiles.shape, F32),
        pltpu.VMEM(coupling_tiles.shape, F32),
        pltpu.VMEM(jacobi_inverse.shape, F32),
        pltpu.VMEM((slot_count, rows_dev), jnp.int32),
        pltpu.VMEM((slot_count, rows_dev), jnp.int32),
        pltpu.SMEM(neighbours.shape, jnp.int32),
        pltpu.VMEM(right_side.shape, F32),
        pltpu.VMEM((n_sub * half_rows, slot_count * chunk), jnp.bfloat16),
        pltpu.VMEM((slot_count * chunk, width), F32),
        pltpu.VMEM((chunk, width), F32),
        pltpu.VMEM((APPLIES, rows_dev, width), F32),
        pltpu.VMEM((APPLIES, n_sub * half_rows, width), F32),
        pltpu.VMEM((APPLIES, slots * n_cols * n_sub * rows_dev, width), F32),
        pltpu.VMEM((APPLIES, SUBLANES, width), F32),
        pltpu.VMEM((APPLIES, peers, SUBLANES, width), F32),
        dma((5 + 2 * (rows_dev // pieces_of(rows_dev)),)),
        dma((APPLIES,)),
        dma((APPLIES,)),
        dma((APPLIES,)),
        dma((APPLIES,)),
    ]
    both = pl.pallas_call(
        functools.partial(kernel, (n_rows, n_cols, n_sub)),
        out_shape=pltpu.VMEM((2 * rows_dev, width), F32),
        in_specs=[hbm] * 7,
        out_specs=vmem,
        scratch_shapes=scratch,
        compiler_params=pltpu.CompilerParams(
            collective_id=0, has_side_effects=True, vmem_limit_bytes=56 * 2**20
        ),
        name="solve",
    )(
        diagonal_tiles,
        coupling_tiles,
        jacobi_inverse,
        column_part.T,
        column_tile.T,
        neighbours,
        right_side,
    )
    return both[:rows_dev], both[rows_dev:]


def solution(mesh):
    in_specs = (
        P(("groups", "rows", "sub"), None, None),
        P(("groups", "rows", "sub"), "cols", None, None),
        P(("groups", "rows", "sub"), "cols"),
        P(("groups", "rows", "sub"), "cols"),
        P("groups", None),
        P(("groups", "rows", "sub"), None),
        P(("groups", "rows", "sub"), None, None),
    )
    out_specs = (P(("groups", "rows", "sub"), None), P(("groups", "rows", "sub"), None))
    return jax.shard_map(
        on_device, mesh=mesh, in_specs=in_specs, out_specs=out_specs, check_vma=False
    )
```

```python
import functools

import jax
import jax.numpy as jnp
from jax import lax
from jax.experimental import pallas as pl
from jax.experimental.pallas import tpu as pltpu
from jax.sharding import PartitionSpec as P

MESH = pl.DeviceIdType.MESH
REACH = 2
APPLIES = 4
SUBLANES = 8
MOST_DOTS = 4
F32 = jnp.float32


def offsets_of(count):
    wanted = {d % count for d in range(-REACH, REACH + 1)} | {count // 2}
    return sorted(wanted)


def pieces_of(rows):
    return 8 if rows % 8 == 0 else 1


def kernel(
    sizes,
    diag_hbm,
    coup_hbm,
    jac_hbm,
    part_hbm,
    tile_hbm,
    near_hbm,
    right_hbm,
    out_ref,
    diag,
    coup,
    jac,
    part_ref,
    tile_ref,
    near_ref,
    right_ref,
    one_hot,
    prod,
    dprod,
    vec,
    landed,
    recv,
    dots,
    dots_recv,
    load_sem,
    send_sem,
    recv_sem,
    dots_send_sem,
    dots_recv_sem,
):
    n_rows, n_cols, n_sub = sizes
    offsets = offsets_of(n_rows)
    slots = len(offsets)
    rows_dev, slot_count, width, _ = coup.shape
    half_rows = slots * rows_dev
    chunk = rows_dev * SUBLANES
    peers = n_rows * n_sub
    unroll = pieces_of(rows_dev)
    row = lax.axis_index("rows")
    col = lax.axis_index("cols")
    sub = lax.axis_index("sub")
    me = row * n_sub + sub

    def piece_loads(g):
        at = pl.ds(g * unroll, unroll)
        return [
            pltpu.make_async_copy(diag_hbm.at[at], diag.at[at], load_sem.at[5 + 2 * g]),
            pltpu.make_async_copy(coup_hbm.at[at], coup.at[at], load_sem.at[6 + 2 * g]),
        ]

    small = [
        pltpu.make_async_copy(part_hbm, part_ref, load_sem.at[0]),
        pltpu.make_async_copy(tile_hbm, tile_ref, load_sem.at[1]),
        pltpu.make_async_copy(near_hbm, near_ref, load_sem.at[2]),
        pltpu.make_async_copy(right_hbm, right_ref, load_sem.at[3]),
    ]
    jac_load = pltpu.make_async_copy(jac_hbm, jac, load_sem.at[4])
    for load in small:
        load.start()
    jac_load.start()
    for g in range(rows_dev // unroll):
        for load in piece_loads(g):
            load.start()

    def partner(slot):
        return lax.rem(row + offsets[slot], n_rows)

    def always(slot):
        return offsets[slot] in (0, n_rows // 2)

    def is_linked(slot):
        return jnp.abs(partner(slot) - row) <= REACH

    def if_linked(slot, act):
        if always(slot):
            act()
        else:
            pl.when(is_linked(slot))(act)

    maybe = [slot for slot in range(slots) if not always(slot)]
    linked_count = slots - len(maybe)
    for slot in maybe:
        linked_count = linked_count + is_linked(slot).astype(jnp.int32)

    def for_linked_count(act):
        if not maybe:
            act(slots)
        for total in range(slots - len(maybe), slots + 1) if maybe else ():
            pl.when(linked_count == total)(functools.partial(act, total))

    def corner(slot, step):
        return {
            "rows": partner(slot),
            "cols": lax.rem(col + step // n_sub, n_cols),
            "sub": lax.rem(sub + step % n_sub, n_sub),
        }

    barrier = pltpu.get_barrier_semaphore()

    def dot_peers():
        for step in range(1, peers):
            peer = lax.rem(me + step, peers)
            yield peer, {"rows": lax.div(peer, n_sub), "cols": col, "sub": lax.rem(peer, n_sub)}

    def from_block(slot, c, s):
        return ((slot * n_cols + c) * n_sub + s) * rows_dev

    per_slot = n_cols * n_sub * rows_dev
    for slot in maybe:
        at = pl.ds(slot * per_slot, per_slot)
        for e in range(APPLIES):
            recv[e, at] = jnp.zeros((per_slot, width), F32)

    far_first = sorted(range(slots), key=lambda s: -min(offsets[s], n_rows - offsets[s]))
    for slot in far_first:
        for step in range(n_sub, n_cols * n_sub):

            def greet(slot=slot, step=step):
                where = corner(slot, step)
                pl.semaphore_signal(barrier, inc=1, device_id=where, device_id_type=MESH)

            if_linked(slot, greet)
    for _, where in dot_peers():
        pl.semaphore_signal(barrier, inc=1, device_id=where, device_id_type=MESH)

    for load in small:
        load.wait()
    part = part_ref[...]
    tile = tile_ref[...]
    target = jnp.full(part.shape, row, jnp.int32)
    for j in range(near_ref.shape[1]):
        target = jnp.where(part == j + 1, near_ref[row, j], target)
    apart = target - row
    apart = jnp.where(apart < 0, apart + n_rows, apart)
    place = jnp.zeros(part.shape, jnp.int32)
    for slot in range(1, slots):
        place = jnp.where(apart == offsets[slot], slot, place)
    landing = place * rows_dev + tile
    for j in range(1, n_sub):
        landing = jnp.where(tile >= j * rows_dev, landing + (half_rows - rows_dev), landing)
    from_row = lax.broadcasted_iota(jnp.int32, (rows_dev, chunk), 0)
    to_lane = lax.broadcasted_iota(jnp.int32, (rows_dev, chunk), 1)
    first = from_row * SUBLANES
    spread = ((to_lane >= first) & (to_lane < first + SUBLANES)).astype(F32)
    spread_landing = jnp.dot(
        landing.astype(F32), spread, precision=lax.Precision.HIGHEST, preferred_element_type=F32
    )
    at_row = lax.broadcasted_iota(jnp.int32, (n_sub * half_rows, chunk), 0).astype(F32)
    for k in range(slot_count):
        hit = (spread_landing[k : k + 1] == at_row).astype(F32)
        one_hot[:, k * chunk : (k + 1) * chunk] = hit.astype(jnp.bfloat16)

    jac_load.wait()

    def turn(r, carry):
        jac[r] = jnp.transpose(jac[r])
        return carry

    lax.fori_loop(0, rows_dev, turn, 0, unroll=4)

    def owner_copy(e, slot, step):
        back = offsets.index(-offsets[slot] % n_rows)
        where = corner(slot, step)
        at = pl.multiple_of(where["sub"] * half_rows + slot * rows_dev, rows_dev)
        to = pl.multiple_of(from_block(back, col, sub), rows_dev)
        return pltpu.make_async_remote_copy(
            src_ref=landed.at[e, pl.ds(at, rows_dev)],
            dst_ref=recv.at[e, pl.ds(to, rows_dev)],
            send_sem=send_sem.at[e],
            recv_sem=recv_sem.at[e],
            device_id=where,
            device_id_type=MESH,
        )

    routes = [(s, c) for s in far_first for c in reversed(range(n_cols * n_sub)) if (s, c) != (0, 0)]

    def each_route(act):
        for slot, step in routes:
            if_linked(slot, functools.partial(act, slot, step))

    def await_rows(sem, count):
        some = recv.at[0, pl.ds(0, count)]
        pltpu.make_async_copy(some, some, sem).wait()

    def await_blocks(sem):
        for_linked_count(lambda total: await_rows(sem, total * per_slot - rows_dev))

    def dots_copy(e, count, where):
        return pltpu.make_async_remote_copy(
            src_ref=dots.at[e, pl.ds(0, count)],
            dst_ref=dots_recv.at[e, me, pl.ds(0, count)],
            send_sem=dots_send_sem.at[e],
            recv_sem=dots_recv_sem.at[e],
            device_id=where,
            device_id_type=MESH,
        )

    def dots_start(e, products):
        count = len(products)
        lines = [jnp.sum(product, axis=0, keepdims=True) for product in products]
        for j, line in enumerate(lines):
            dots[e, j : j + 1] = line
        for _, where in dot_peers():
            dots_copy(e, count, where).start()
        for j, line in enumerate(lines):
            dots_recv[e, me, j : j + 1] = line

    def dots_finish(e, count):
        await_rows(dots_recv_sem.at[e], (peers - 1) * count)
        lines = jnp.sum(dots_recv[e, :, :count], axis=0)
        total = jnp.sum(lines, axis=1, keepdims=True)
        return [jnp.broadcast_to(total[j : j + 1], (1, width)) for j in range(count)]

    def fold(product):
        return jnp.sum(product.reshape(width // SUBLANES, SUBLANES, width), axis=0)

    def send_products(e, value, products=()):
        if e > 0:
            vec[e] = value
        if products:
            dots_start(e - 1, products)

        def some_rows(g, carry):
            if e == 0:
                for load in piece_loads(g):
                    load.wait()
            for u in range(unroll):
                r = g * unroll + u
                line = vec[e, pl.ds(r, 1)] if e > 0 else right_ref[pl.ds(r, 1)]
                hat = jnp.sum(jac[r] * line, axis=1, keepdims=True)
                hat = jnp.broadcast_to(hat, (width, width))
                for k in range(slot_count):
                    at = pl.multiple_of(k * chunk + r * SUBLANES, SUBLANES)
                    prod[pl.ds(at, SUBLANES)] = fold(coup[r, k] * hat)
                dprod[pl.ds(pl.multiple_of(r * SUBLANES, SUBLANES), SUBLANES)] = fold(diag[r] * hat)
            return carry

        lax.fori_loop(0, rows_dev // unroll, some_rows, 0)
        rest = prod[...]
        out = None
        for _ in range(3):
            piece = rest.astype(jnp.bfloat16)
            rest = rest - piece.astype(F32)
            term = jnp.dot(one_hot[...], piece, preferred_element_type=F32)
            out = term if out is None else out + term
        landed[e] = out
        if e == 0:
            greetings = peers - 1 + (n_cols - 1) * n_sub * linked_count
            pl.semaphore_wait(barrier, greetings)
        each_route(lambda slot, step: owner_copy(e, slot, step).start())

    def own_products(e):
        at = pl.multiple_of(from_block(0, col, sub), rows_dev)
        from_at = pl.multiple_of(sub * half_rows, rows_dev)
        recv[e, pl.ds(at, rows_dev)] = landed[e, pl.ds(from_at, rows_dev)]
        return jnp.sum(dprod[...].reshape(rows_dev, SUBLANES, width), axis=1)

    def gather_products(e, own):
        await_blocks(recv_sem.at[e])
        for b in range(slots * n_cols * n_sub):
            own = own + recv[e, b * rows_dev : (b + 1) * rows_dev]
        return own

    shadow = right_ref[...]
    send_products(0, shadow)
    own = own_products(0)
    image = gather_products(0, own)

    send_products(1, image, [shadow * shadow, shadow * image])
    own = own_products(1)
    rho, shadow_image = dots_finish(0, 2)
    alpha = rho / shadow_image
    half = shadow - alpha * image
    second = gather_products(1, own)
    twice = image - alpha * second

    send_products(2, twice, [twice * half, twice * twice, shadow * half, shadow * twice])
    own = own_products(2)
    cross, square, shadow_half, shadow_twice = dots_finish(1, 4)
    omega = cross / square
    rho_next = shadow_half - omega * shadow_twice
    beta = rho_next / rho * (alpha / omega)
    residual = half - omega * twice
    search = residual + beta * (shadow - omega * image)
    known = twice + beta * (image - omega * second)
    third = gather_products(2, own)
    residual_image = twice - omega * third
    image = known - omega * third

    send_products(3, image, [shadow * image])
    own = own_products(3)
    alpha_next = rho_next / dots_finish(2, 1)[0]
    half_next = residual - alpha_next * image
    fourth = gather_products(3, own)
    twice = residual_image - alpha_next * fourth
    dots_start(3, [twice * half_next, twice * twice])

    vec[0] = alpha * shadow + omega * half + alpha_next * search
    vec[1] = half_next
    at_lane = lax.broadcasted_iota(jnp.int32, (width, width), 1)

    def hats(r, carry):
        for j in range(2):
            hat = jnp.sum(jac[r] * vec[j, pl.ds(r, 1)], axis=1, keepdims=True)
            carry = jnp.where(at_lane == j * rows_dev + r, hat, carry)
        return carry

    hat = lax.fori_loop(0, rows_dev, hats, jnp.zeros((width, width), F32), unroll=4)
    hat = jnp.transpose(hat)
    for e in range(APPLIES):
        await_blocks(send_sem.at[e])
    cross, square = dots_finish(3, 2)
    omega = cross / square
    out_ref[:rows_dev] = hat[:rows_dev] + omega * hat[rows_dev : 2 * rows_dev]
    out_ref[rows_dev:] = half_next - omega * twice
    for e, count in enumerate((2, 4, 1, 2)):
        await_rows(dots_send_sem.at[e], (peers - 1) * count)


def on_device(
    diagonal_tiles, coupling_tiles, column_part, column_tile, neighbours, right_side, jacobi_inverse
):
    n_rows, n_cols, n_sub = (lax.axis_size(a) for a in ("rows", "cols", "sub"))
    slots = len(offsets_of(n_rows))
    rows_dev, slot_count, width, _ = coupling_tiles.shape
    half_rows = slots * rows_dev
    chunk = rows_dev * SUBLANES
    peers = n_rows * n_sub
    hbm = pl.BlockSpec(memory_space=pl.ANY)
    vmem = pl.BlockSpec(memory_space=pltpu.VMEM)
    dma = pltpu.SemaphoreType.DMA
    scratch = [
        pltpu.VMEM(diagonal_tiles.shape, F32),
        pltpu.VMEM(coupling_tiles.shape, F32),
        pltpu.VMEM(jacobi_inverse.shape, F32),
        pltpu.VMEM((slot_count, rows_dev), jnp.int32),
        pltpu.VMEM((slot_count, rows_dev), jnp.int32),
        pltpu.SMEM(neighbours.shape, jnp.int32),
        pltpu.VMEM(right_side.shape, F32),
        pltpu.VMEM((n_sub * half_rows, slot_count * chunk), jnp.bfloat16),
        pltpu.VMEM((slot_count * chunk, width), F32),
        pltpu.VMEM((chunk, width), F32),
        pltpu.VMEM((APPLIES, rows_dev, width), F32),
        pltpu.VMEM((APPLIES, n_sub * half_rows, width), F32),
        pltpu.VMEM((APPLIES, slots * n_cols * n_sub * rows_dev, width), F32),
        pltpu.VMEM((APPLIES, SUBLANES, width), F32),
        pltpu.VMEM((APPLIES, peers, SUBLANES, width), F32),
        dma((5 + 2 * (rows_dev // pieces_of(rows_dev)),)),
        dma((APPLIES,)),
        dma((APPLIES,)),
        dma((APPLIES,)),
        dma((APPLIES,)),
    ]
    both = pl.pallas_call(
        functools.partial(kernel, (n_rows, n_cols, n_sub)),
        out_shape=pltpu.VMEM((2 * rows_dev, width), F32),
        in_specs=[hbm] * 7,
        out_specs=vmem,
        scratch_shapes=scratch,
        compiler_params=pltpu.CompilerParams(
            collective_id=0, has_side_effects=True, vmem_limit_bytes=56 * 2**20
        ),
        name="solve",
    )(
        diagonal_tiles,
        coupling_tiles,
        jacobi_inverse,
        column_part.T,
        column_tile.T,
        neighbours,
        right_side,
    )
    return both[:rows_dev], both[rows_dev:]


def solution(mesh):
    in_specs = (
        P(("groups", "rows", "sub"), None, None),
        P(("groups", "rows", "sub"), "cols", None, None),
        P(("groups", "rows", "sub"), "cols"),
        P(("groups", "rows", "sub"), "cols"),
        P("groups", None),
        P(("groups", "rows", "sub"), None),
        P(("groups", "rows", "sub"), None, None),
    )
    out_specs = (P(("groups", "rows", "sub"), None), P(("groups", "rows", "sub"), None))
    return jax.shard_map(
        on_device, mesh=mesh, in_specs=in_specs, out_specs=out_specs, check_vma=False
    )
```

```python
import functools

import jax
import jax.numpy as jnp
from jax import lax
from jax.experimental import pallas as pl
from jax.experimental.pallas import tpu as pltpu
from jax.sharding import PartitionSpec as P

MESH = pl.DeviceIdType.MESH
REACH = 2
APPLIES = 4
SUBLANES = 8
MOST_DOTS = 4
F32 = jnp.float32


def offsets_of(count):
    wanted = {d % count for d in range(-REACH, REACH + 1)} | {count // 2}
    return sorted(wanted)


def pieces_of(rows):
    return 8 if rows % 8 == 0 else 1


def kernel(
    sizes,
    diag_hbm,
    coup_hbm,
    jac_hbm,
    part_hbm,
    tile_hbm,
    near_hbm,
    right_hbm,
    out_ref,
    diag,
    coup,
    jac,
    part_ref,
    tile_ref,
    near_ref,
    right_ref,
    one_hot,
    prod,
    dprod,
    vec,
    landed,
    recv,
    hub_recv,
    kept,
    ends,
    dots,
    dots_recv,
    load_sem,
    send_sem,
    recv_sem,
    dots_send_sem,
    dots_recv_sem,
    core_sem,
):
    n_rows, n_cols, n_sub = sizes
    offsets = offsets_of(n_rows)
    slots = len(offsets)
    rows_dev, slot_count, width, _ = coup.shape
    part_rows = n_sub * rows_dev
    chunk = rows_dev * SUBLANES
    peers = n_rows * n_sub
    hub = n_sub - 1
    last = APPLIES - 1
    unroll = pieces_of(rows_dev)
    row = lax.axis_index("rows")
    col = lax.axis_index("cols")
    sub = lax.axis_index("sub")
    me = row * n_sub + sub

    def piece_loads(g):
        at = pl.ds(g * unroll, unroll)
        return [
            pltpu.make_async_copy(diag_hbm.at[at], diag.at[at], load_sem.at[5 + 2 * g]),
            pltpu.make_async_copy(coup_hbm.at[at], coup.at[at], load_sem.at[6 + 2 * g]),
        ]

    small = [
        pltpu.make_async_copy(part_hbm, part_ref, load_sem.at[0]),
        pltpu.make_async_copy(tile_hbm, tile_ref, load_sem.at[1]),
        pltpu.make_async_copy(near_hbm, near_ref, load_sem.at[2]),
        pltpu.make_async_copy(right_hbm, right_ref, load_sem.at[3]),
    ]
    jac_load = pltpu.make_async_copy(jac_hbm, jac, load_sem.at[4])
    for load in small:
        load.start()
    jac_load.start()
    for g in range(rows_dev // unroll):
        for load in piece_loads(g):
            load.start()

    def partner(slot):
        return lax.rem(row + offsets[slot], n_rows)

    def always(slot):
        return offsets[slot] in (0, n_rows // 2)

    def is_linked(slot):
        return jnp.abs(partner(slot) - row) <= REACH

    def if_linked(slot, act):
        if always(slot):
            act()
        else:
            pl.when(is_linked(slot))(act)

    maybe = [slot for slot in range(slots) if not always(slot)]
    linked_count = slots - len(maybe)
    for slot in maybe:
        linked_count = linked_count + is_linked(slot).astype(jnp.int32)

    def for_linked_count(act):
        if not maybe:
            act(slots)
        for total in range(slots - len(maybe), slots + 1) if maybe else ():
            pl.when(linked_count == total)(functools.partial(act, total))

    def corner(slot, step):
        return {
            "rows": partner(slot),
            "cols": lax.rem(col + step // n_sub, n_cols),
            "sub": lax.rem(sub + step % n_sub, n_sub),
        }

    barrier = pltpu.get_barrier_semaphore()

    def dot_peers():
        for step in range(1, peers):
            peer = lax.rem(me + step, peers)
            yield peer, {"rows": lax.div(peer, n_sub), "cols": col, "sub": lax.rem(peer, n_sub)}

    def from_block(slot, c, s):
        return ((slot * n_cols + c) * n_sub + s) * rows_dev

    per_slot = n_cols * n_sub * rows_dev
    for slot in maybe:
        at = pl.ds(slot * per_slot, per_slot)
        for e in range(last):
            recv[e, at] = jnp.zeros((per_slot, width), F32)
        hub_recv[slot * per_slot * n_sub : (slot + 1) * per_slot * n_sub] = jnp.zeros(
            (per_slot * n_sub, width), F32
        )

    far_first = sorted(range(slots), key=lambda s: -min(offsets[s], n_rows - offsets[s]))
    for slot in far_first:
        for step in range(n_sub, n_cols * n_sub):

            def greet(slot=slot, step=step):
                where = corner(slot, step)
                pl.semaphore_signal(barrier, inc=1, device_id=where, device_id_type=MESH)

            if_linked(slot, greet)
    for _, where in dot_peers():
        pl.semaphore_signal(barrier, inc=1, device_id=where, device_id_type=MESH)

    for load in small:
        load.wait()
    part = part_ref[...]
    tile = tile_ref[...]
    target = jnp.full(part.shape, row, jnp.int32)
    for j in range(near_ref.shape[1]):
        target = jnp.where(part == j + 1, near_ref[row, j], target)
    apart = target - row
    apart = jnp.where(apart < 0, apart + n_rows, apart)
    place = jnp.zeros(part.shape, jnp.int32)
    for slot in range(1, slots):
        place = jnp.where(apart == offsets[slot], slot, place)
    landing = place * part_rows + tile
    from_row = lax.broadcasted_iota(jnp.int32, (rows_dev, chunk), 0)
    to_lane = lax.broadcasted_iota(jnp.int32, (rows_dev, chunk), 1)
    first = from_row * SUBLANES
    spread = ((to_lane >= first) & (to_lane < first + SUBLANES)).astype(F32)
    spread_landing = jnp.dot(
        landing.astype(F32), spread, precision=lax.Precision.HIGHEST, preferred_element_type=F32
    )
    at_row = lax.broadcasted_iota(jnp.int32, (slots * part_rows, chunk), 0).astype(F32)
    for k in range(slot_count):
        hit = (spread_landing[k : k + 1] == at_row).astype(F32)
        one_hot[:, k * chunk : (k + 1) * chunk] = hit.astype(jnp.bfloat16)

    jac_load.wait()

    def turn(r, carry):
        jac[r] = jnp.transpose(jac[r])
        return carry

    lax.fori_loop(0, rows_dev, turn, 0, unroll=4)

    def owner_copy(e, slot, step):
        back = offsets.index(-offsets[slot] % n_rows)
        where = corner(slot, step)
        at = pl.multiple_of(slot * part_rows + where["sub"] * rows_dev, rows_dev)
        to = pl.multiple_of(from_block(back, col, sub), rows_dev)
        return pltpu.make_async_remote_copy(
            src_ref=landed.at[e, pl.ds(at, rows_dev)],
            dst_ref=recv.at[e, pl.ds(to, rows_dev)],
            send_sem=send_sem.at[e],
            recv_sem=recv_sem.at[e],
            device_id=where,
            device_id_type=MESH,
        )

    routes = [(s, c) for s in far_first for c in reversed(range(n_cols * n_sub)) if (s, c) != (0, 0)]

    def each_route(act):
        for slot, step in routes:
            if_linked(slot, functools.partial(act, slot, step))

    def hub_copy(slot, across):
        back = offsets.index(-offsets[slot] % n_rows)
        to = pl.multiple_of(from_block(back, col, sub) * n_sub, part_rows)
        return pltpu.make_async_remote_copy(
            src_ref=landed.at[last, pl.ds(slot * part_rows, part_rows)],
            dst_ref=hub_recv.at[pl.ds(to, part_rows)],
            send_sem=send_sem.at[last],
            recv_sem=recv_sem.at[last],
            device_id={
                "rows": partner(slot),
                "cols": lax.rem(col + across, n_cols),
                "sub": jnp.int32(hub),
            },
            device_id_type=MESH,
        )

    def core_copy(ref, index, to, which):
        return pltpu.make_async_remote_copy(
            src_ref=ref.at[index],
            dst_ref=ref.at[index],
            send_sem=core_sem.at[2 * which],
            recv_sem=core_sem.at[2 * which + 1],
            device_id={"rows": row, "cols": col, "sub": jnp.int32(to)},
            device_id_type=MESH,
        )

    def at_hub(act):
        pl.when(sub == hub)(act)

    def off_hub(act):
        pl.when(sub != hub)(act)

    def await_rows(sem, count):
        some = hub_recv.at[pl.ds(0, count)]
        pltpu.make_async_copy(some, some, sem).wait()

    def await_blocks(sem):
        for_linked_count(lambda total: await_rows(sem, total * per_slot - rows_dev))

    def dots_copy(e, count, where):
        return pltpu.make_async_remote_copy(
            src_ref=dots.at[e, pl.ds(0, count)],
            dst_ref=dots_recv.at[e, me, pl.ds(0, count)],
            send_sem=dots_send_sem.at[e],
            recv_sem=dots_recv_sem.at[e],
            device_id=where,
            device_id_type=MESH,
        )

    def dots_start(e, products):
        count = len(products)
        lines = [jnp.sum(product, axis=0, keepdims=True) for product in products]
        for j, line in enumerate(lines):
            dots[e, j : j + 1] = line
        for _, where in dot_peers():
            dots_copy(e, count, where).start()
        for j, line in enumerate(lines):
            dots_recv[e, me, j : j + 1] = line

    def dots_finish(e, count):
        await_rows(dots_recv_sem.at[e], (peers - 1) * count)
        lines = jnp.sum(dots_recv[e, :, :count], axis=0)
        total = jnp.sum(lines, axis=1, keepdims=True)
        return [jnp.broadcast_to(total[j : j + 1], (1, width)) for j in range(count)]

    def fold(product):
        return jnp.sum(product.reshape(width // SUBLANES, SUBLANES, width), axis=0)

    def send_products(e, value, products=()):
        if e > 0:
            vec[e] = value
        if products:
            dots_start(e - 1, products)

        def some_rows(g, carry):
            if e == 0:
                for load in piece_loads(g):
                    load.wait()
            for u in range(unroll):
                r = g * unroll + u
                line = vec[e, pl.ds(r, 1)] if e > 0 else right_ref[pl.ds(r, 1)]
                hat = jnp.sum(jac[r] * line, axis=1, keepdims=True)
                hat = jnp.broadcast_to(hat, (width, width))
                for k in range(slot_count):
                    at = pl.multiple_of(k * chunk + r * SUBLANES, SUBLANES)
                    prod[pl.ds(at, SUBLANES)] = fold(coup[r, k] * hat)
                dprod[pl.ds(pl.multiple_of(r * SUBLANES, SUBLANES), SUBLANES)] = fold(diag[r] * hat)
            return carry

        lax.fori_loop(0, rows_dev // unroll, some_rows, 0)
        rest = prod[...]
        out = None
        for _ in range(3):
            piece = rest.astype(jnp.bfloat16)
            rest = rest - piece.astype(F32)
            term = jnp.dot(one_hot[...], piece, preferred_element_type=F32)
            out = term if out is None else out + term
        landed[e] = out
        if e == last:
            at = pl.multiple_of(sub * rows_dev, rows_dev)
            own = jnp.sum(dprod[...].reshape(rows_dev, SUBLANES, width), axis=1)
            own = jnp.where(col == 0, own, 0.0)
            landed[e, pl.ds(at, rows_dev)] = landed[e, pl.ds(at, rows_dev)] + own
            for slot in far_first:
                for across in reversed(range(n_cols)):
                    send = functools.partial(lambda s, a: hub_copy(s, a).start(), slot, across)
                    if (slot, across) == (0, 0):
                        off_hub(send)
                    else:
                        if_linked(slot, send)
            return
        if e == 0:
            greetings = peers - 1 + (n_cols - 1) * n_sub * linked_count
            pl.semaphore_wait(barrier, greetings)
        each_route(lambda slot, step: owner_copy(e, slot, step).start())

    def own_products(e):
        at = pl.multiple_of(from_block(0, col, sub), rows_dev)
        from_at = pl.multiple_of(sub * rows_dev, rows_dev)
        recv[e, pl.ds(at, rows_dev)] = landed[e, pl.ds(from_at, rows_dev)]
        return jnp.sum(dprod[...].reshape(rows_dev, SUBLANES, width), axis=1)

    def gather_products(e, own):
        await_blocks(recv_sem.at[e])
        for b in range(slots * n_cols * n_sub):
            own = own + recv[e, b * rows_dev : (b + 1) * rows_dev]
        return own

    shadow = right_ref[...]
    send_products(0, shadow)
    own = own_products(0)
    image = gather_products(0, own)

    send_products(1, image, [shadow * shadow, shadow * image])
    own = own_products(1)
    rho, shadow_image = dots_finish(0, 2)
    alpha = rho / shadow_image
    half = shadow - alpha * image
    second = gather_products(1, own)
    twice = image - alpha * second

    send_products(2, twice, [twice * half, twice * twice, shadow * half, shadow * twice])
    own = own_products(2)
    cross, square, shadow_half, shadow_twice = dots_finish(1, 4)
    omega = cross / square
    rho_next = shadow_half - omega * shadow_twice
    beta = rho_next / rho * (alpha / omega)
    residual = half - omega * twice
    search = residual + beta * (shadow - omega * image)
    known = twice + beta * (image - omega * second)
    third = gather_products(2, own)
    residual_image = twice - omega * third
    image = known - omega * third
    kept[sub, 0] = residual_image
    kept[sub, 1] = residual
    kept[sub, 2] = image

    @off_hub
    def _():
        core_copy(kept, sub, hub, 0).start()

    send_products(3, image, [shadow * image])
    alpha_next = rho_next / dots_finish(2, 1)[0]
    half_next = residual - alpha_next * image

    @at_hub
    def _():
        at = pl.multiple_of(from_block(0, col, sub) * n_sub, part_rows)
        hub_recv[pl.ds(at, part_rows)] = landed[last, :part_rows]
        if n_sub > 1:
            await_rows(core_sem.at[1], (n_sub - 1) * 3 * rows_dev)
        for_linked_count(
            lambda total: await_rows(recv_sem.at[last], (total * n_cols * n_sub - 1) * part_rows)
        )
        fourth = hub_recv[:part_rows]
        for b in range(1, slots * n_cols * n_sub):
            fourth = fourth + hub_recv[b * part_rows : (b + 1) * part_rows]
        cross = jnp.zeros((rows_dev, width), F32)
        square = jnp.zeros((rows_dev, width), F32)
        for t in range(n_sub):
            end = kept[t, 0] - alpha_next * fourth[t * rows_dev : (t + 1) * rows_dev]
            cross = cross + end * (kept[t, 1] - alpha_next * kept[t, 2])
            square = square + end * end
            ends[t] = end
        for j, product in enumerate((cross, square)):
            dots[last, j : j + 1] = jnp.sum(product, axis=0, keepdims=True)
        for _, where in dot_peers():
            dots_copy(last, 2, where).start()
        for t in range(hub):
            core_copy(ends, t, t, 1).start()
        dots_recv[last, me, :2] = dots[last, :2]

    vec[0] = alpha * shadow + omega * half + alpha_next * search
    vec[1] = half_next
    at_lane = lax.broadcasted_iota(jnp.int32, (width, width), 1)

    def hats(r, carry):
        for j in range(2):
            hat = jnp.sum(jac[r] * vec[j, pl.ds(r, 1)], axis=1, keepdims=True)
            carry = jnp.where(at_lane == j * rows_dev + r, hat, carry)
        return carry

    hat = lax.fori_loop(0, rows_dev, hats, jnp.zeros((width, width), F32), unroll=4)
    hat = jnp.transpose(hat)
    for e in range(last):
        await_blocks(send_sem.at[e])
    for e, count in enumerate((2, 4, 1)):
        await_rows(dots_send_sem.at[e], (peers - 1) * count)

    @at_hub
    def _():
        for_linked_count(
            lambda total: await_rows(send_sem.at[last], (total * n_cols - 1) * part_rows)
        )
        await_rows(dots_send_sem.at[last], (peers - 1) * 2)
        if hub > 0:
            await_rows(core_sem.at[2], hub * rows_dev)
        await_rows(dots_recv_sem.at[last], (n_rows - 1) * 2)

    @off_hub
    def _():
        for_linked_count(lambda total: await_rows(send_sem.at[last], total * n_cols * part_rows))
        await_rows(core_sem.at[0], 3 * rows_dev)
        await_rows(core_sem.at[3], rows_dev)
        await_rows(dots_recv_sem.at[last], n_rows * 2)

    lines = dots_recv[last, hub, :2]
    for r in range(1, n_rows):
        lines = lines + dots_recv[last, r * n_sub + hub, :2]
    total = jnp.sum(lines, axis=1, keepdims=True)
    omega = jnp.broadcast_to(total[:1], (1, width)) / jnp.broadcast_to(total[1:], (1, width))
    out_ref[:rows_dev] = hat[:rows_dev] + omega * hat[rows_dev : 2 * rows_dev]
    out_ref[rows_dev:] = half_next - omega * ends[sub]


def on_device(
    diagonal_tiles, coupling_tiles, column_part, column_tile, neighbours, right_side, jacobi_inverse
):
    n_rows, n_cols, n_sub = (lax.axis_size(a) for a in ("rows", "cols", "sub"))
    slots = len(offsets_of(n_rows))
    rows_dev, slot_count, width, _ = coupling_tiles.shape
    part_rows = n_sub * rows_dev
    chunk = rows_dev * SUBLANES
    peers = n_rows * n_sub
    hbm = pl.BlockSpec(memory_space=pl.ANY)
    vmem = pl.BlockSpec(memory_space=pltpu.VMEM)
    dma = pltpu.SemaphoreType.DMA
    scratch = [
        pltpu.VMEM(diagonal_tiles.shape, F32),
        pltpu.VMEM(coupling_tiles.shape, F32),
        pltpu.VMEM(jacobi_inverse.shape, F32),
        pltpu.VMEM((slot_count, rows_dev), jnp.int32),
        pltpu.VMEM((slot_count, rows_dev), jnp.int32),
        pltpu.SMEM(neighbours.shape, jnp.int32),
        pltpu.VMEM(right_side.shape, F32),
        pltpu.VMEM((slots * part_rows, slot_count * chunk), jnp.bfloat16),
        pltpu.VMEM((slot_count * chunk, width), F32),
        pltpu.VMEM((chunk, width), F32),
        pltpu.VMEM((APPLIES, rows_dev, width), F32),
        pltpu.VMEM((APPLIES, slots * part_rows, width), F32),
        pltpu.VMEM((APPLIES - 1, slots * n_cols * part_rows, width), F32),
        pltpu.VMEM((slots * n_cols * n_sub * part_rows, width), F32),
        pltpu.VMEM((n_sub, 3, rows_dev, width), F32),
        pltpu.VMEM((n_sub, rows_dev, width), F32),
        pltpu.VMEM((APPLIES, SUBLANES, width), F32),
        pltpu.VMEM((APPLIES, peers, SUBLANES, width), F32),
        dma((5 + 2 * (rows_dev // pieces_of(rows_dev)),)),
        dma((APPLIES,)),
        dma((APPLIES,)),
        dma((APPLIES,)),
        dma((APPLIES,)),
        dma((4,)),
    ]
    both = pl.pallas_call(
        functools.partial(kernel, (n_rows, n_cols, n_sub)),
        out_shape=pltpu.VMEM((2 * rows_dev, width), F32),
        in_specs=[hbm] * 7,
        out_specs=vmem,
        scratch_shapes=scratch,
        compiler_params=pltpu.CompilerParams(
            collective_id=0, has_side_effects=True, vmem_limit_bytes=56 * 2**20
        ),
        name="solve",
    )(
        diagonal_tiles,
        coupling_tiles,
        jacobi_inverse,
        column_part.T,
        column_tile.T,
        neighbours,
        right_side,
    )
    return both[:rows_dev], both[rows_dev:]


def solution(mesh):
    in_specs = (
        P(("groups", "rows", "sub"), None, None),
        P(("groups", "rows", "sub"), "cols", None, None),
        P(("groups", "rows", "sub"), "cols"),
        P(("groups", "rows", "sub"), "cols"),
        P("groups", None),
        P(("groups", "rows", "sub"), None),
        P(("groups", "rows", "sub"), None, None),
    )
    out_specs = (P(("groups", "rows", "sub"), None), P(("groups", "rows", "sub"), None))
    return jax.shard_map(
        on_device, mesh=mesh, in_specs=in_specs, out_specs=out_specs, check_vma=False
    )
```

```python
import functools

import jax
import jax.numpy as jnp
from jax import lax
from jax.experimental import pallas as pl
from jax.experimental.pallas import tpu as pltpu
from jax.sharding import PartitionSpec as P

MESH = pl.DeviceIdType.MESH
REACH = 2
APPLIES = 4
SUBLANES = 8
MOST_DOTS = 4
F32 = jnp.float32


def offsets_of(count):
    wanted = {d % count for d in range(-REACH, REACH + 1)} | {count // 2}
    return sorted(wanted)


def pieces_of(rows):
    return 8 if rows % 8 == 0 else 1


def kernel(
    sizes,
    diag_hbm,
    coup_hbm,
    jac_hbm,
    part_hbm,
    tile_hbm,
    near_hbm,
    right_hbm,
    out_ref,
    diag,
    coup,
    jac,
    part_ref,
    tile_ref,
    near_ref,
    right_ref,
    one_hot,
    prod,
    dprod,
    vec,
    landed,
    recv,
    hub_recv,
    kept,
    ends,
    dots,
    dots_recv,
    load_sem,
    send_sem,
    recv_sem,
    dots_send_sem,
    dots_recv_sem,
    core_sem,
):
    n_rows, n_cols, n_sub = sizes
    offsets = offsets_of(n_rows)
    slots = len(offsets)
    rows_dev, slot_count, width, _ = coup.shape
    part_rows = n_sub * rows_dev
    chunk = rows_dev * SUBLANES
    peers = n_rows * n_sub
    hub = n_sub - 1
    last = APPLIES - 1
    unroll = pieces_of(rows_dev)
    row = lax.axis_index("rows")
    col = lax.axis_index("cols")
    sub = lax.axis_index("sub")
    me = row * n_sub + sub

    def piece_loads(g):
        at = pl.ds(g * unroll, unroll)
        return [
            pltpu.make_async_copy(diag_hbm.at[at], diag.at[at], load_sem.at[5 + 2 * g]),
            pltpu.make_async_copy(coup_hbm.at[at], coup.at[at], load_sem.at[6 + 2 * g]),
        ]

    small = [
        pltpu.make_async_copy(part_hbm, part_ref, load_sem.at[0]),
        pltpu.make_async_copy(tile_hbm, tile_ref, load_sem.at[1]),
        pltpu.make_async_copy(near_hbm, near_ref, load_sem.at[2]),
        pltpu.make_async_copy(right_hbm, right_ref, load_sem.at[3]),
    ]
    jac_load = pltpu.make_async_copy(jac_hbm, jac, load_sem.at[4])
    for load in small:
        load.start()
    jac_load.start()
    for g in range(rows_dev // unroll):
        for load in piece_loads(g):
            load.start()

    def partner(slot):
        return lax.rem(row + offsets[slot], n_rows)

    def always(slot):
        return offsets[slot] in (0, n_rows // 2)

    def is_linked(slot):
        return jnp.abs(partner(slot) - row) <= REACH

    def if_linked(slot, act):
        if always(slot):
            act()
        else:
            pl.when(is_linked(slot))(act)

    maybe = [slot for slot in range(slots) if not always(slot)]
    linked_count = slots - len(maybe)
    for slot in maybe:
        linked_count = linked_count + is_linked(slot).astype(jnp.int32)

    def for_linked_count(act):
        if not maybe:
            act(slots)
        for total in range(slots - len(maybe), slots + 1) if maybe else ():
            pl.when(linked_count == total)(functools.partial(act, total))

    def corner(slot, step):
        return {
            "rows": partner(slot),
            "cols": lax.rem(col + step // n_sub, n_cols),
            "sub": lax.rem(sub + step % n_sub, n_sub),
        }

    barrier = pltpu.get_barrier_semaphore()

    def dot_peers():
        for step in range(1, peers):
            peer = lax.rem(me + step, peers)
            yield peer, {"rows": lax.div(peer, n_sub), "cols": col, "sub": lax.rem(peer, n_sub)}

    def from_block(slot, c, s):
        return ((slot * n_cols + c) * n_sub + s) * rows_dev

    per_slot = n_cols * n_sub * rows_dev
    for slot in maybe:
        at = pl.ds(slot * per_slot, per_slot)
        for e in range(last):
            recv[e, at] = jnp.zeros((per_slot, width), F32)
        hub_recv[slot * per_slot * n_sub : (slot + 1) * per_slot * n_sub] = jnp.zeros(
            (per_slot * n_sub, width), F32
        )

    far_first = sorted(range(slots), key=lambda s: -min(offsets[s], n_rows - offsets[s]))
    for slot in far_first:
        for step in range(n_sub, n_cols * n_sub):

            def greet(slot=slot, step=step):
                where = corner(slot, step)
                pl.semaphore_signal(barrier, inc=1, device_id=where, device_id_type=MESH)

            if_linked(slot, greet)
    for _, where in dot_peers():
        pl.semaphore_signal(barrier, inc=1, device_id=where, device_id_type=MESH)

    for load in small:
        load.wait()
    part = part_ref[...]
    tile = tile_ref[...]
    target = jnp.full(part.shape, row, jnp.int32)
    for j in range(near_ref.shape[1]):
        target = jnp.where(part == j + 1, near_ref[row, j], target)
    apart = target - row
    apart = jnp.where(apart < 0, apart + n_rows, apart)
    place = jnp.zeros(part.shape, jnp.int32)
    for slot in range(1, slots):
        place = jnp.where(apart == offsets[slot], slot, place)
    landing = place * part_rows + tile
    from_row = lax.broadcasted_iota(jnp.int32, (rows_dev, chunk), 0)
    to_lane = lax.broadcasted_iota(jnp.int32, (rows_dev, chunk), 1)
    first = from_row * SUBLANES
    spread = ((to_lane >= first) & (to_lane < first + SUBLANES)).astype(F32)
    spread_landing = jnp.dot(
        landing.astype(F32), spread, precision=lax.Precision.HIGHEST, preferred_element_type=F32
    )
    at_row = lax.broadcasted_iota(jnp.int32, (slots * part_rows, chunk), 0).astype(F32)
    for k in range(slot_count):
        hit = (spread_landing[k : k + 1] == at_row).astype(F32)
        one_hot[:, k * chunk : (k + 1) * chunk] = hit.astype(jnp.bfloat16)

    jac_load.wait()

    def turn(r, carry):
        jac[r] = jnp.transpose(jac[r])
        return carry

    lax.fori_loop(0, rows_dev, turn, 0, unroll=4)

    def owner_copy(e, slot, step):
        back = offsets.index(-offsets[slot] % n_rows)
        where = corner(slot, step)
        at = pl.multiple_of(slot * part_rows + where["sub"] * rows_dev, rows_dev)
        to = pl.multiple_of(from_block(back, col, sub), rows_dev)
        return pltpu.make_async_remote_copy(
            src_ref=landed.at[e, pl.ds(at, rows_dev)],
            dst_ref=recv.at[e, pl.ds(to, rows_dev)],
            send_sem=send_sem.at[e],
            recv_sem=recv_sem.at[e],
            device_id=where,
            device_id_type=MESH,
        )

    routes = [(s, c) for s in far_first for c in reversed(range(n_cols * n_sub)) if (s, c) != (0, 0)]

    def each_route(act):
        for slot, step in routes:
            if_linked(slot, functools.partial(act, slot, step))

    def hub_copy(slot, across):
        back = offsets.index(-offsets[slot] % n_rows)
        to = pl.multiple_of(from_block(back, col, sub) * n_sub, part_rows)
        return pltpu.make_async_remote_copy(
            src_ref=landed.at[last, pl.ds(slot * part_rows, part_rows)],
            dst_ref=hub_recv.at[pl.ds(to, part_rows)],
            send_sem=send_sem.at[last],
            recv_sem=recv_sem.at[last],
            device_id={
                "rows": partner(slot),
                "cols": lax.rem(col + across, n_cols),
                "sub": jnp.int32(hub),
            },
            device_id_type=MESH,
        )

    def core_copy(ref, index, to, which):
        return pltpu.make_async_remote_copy(
            src_ref=ref.at[index],
            dst_ref=ref.at[index],
            send_sem=core_sem.at[2 * which],
            recv_sem=core_sem.at[2 * which + 1],
            device_id={"rows": row, "cols": col, "sub": jnp.int32(to)},
            device_id_type=MESH,
        )

    def at_hub(act):
        pl.when(sub == hub)(act)

    def off_hub(act):
        pl.when(sub != hub)(act)

    def await_rows(sem, count):
        some = hub_recv.at[pl.ds(0, count)]
        pltpu.make_async_copy(some, some, sem).wait()

    def await_blocks(sem):
        for_linked_count(lambda total: await_rows(sem, total * per_slot - rows_dev))

    def dots_copy(e, count, where):
        return pltpu.make_async_remote_copy(
            src_ref=dots.at[e, pl.ds(0, count)],
            dst_ref=dots_recv.at[e, me, pl.ds(0, count)],
            send_sem=dots_send_sem.at[e],
            recv_sem=dots_recv_sem.at[e],
            device_id=where,
            device_id_type=MESH,
        )

    def dots_start(e, products):
        count = len(products)
        lines = [jnp.sum(product, axis=0, keepdims=True) for product in products]
        for j, line in enumerate(lines):
            dots[e, j : j + 1] = line
        for _, where in dot_peers():
            dots_copy(e, count, where).start()
        for j, line in enumerate(lines):
            dots_recv[e, me, j : j + 1] = line

    def dots_finish(e, count):
        await_rows(dots_recv_sem.at[e], (peers - 1) * count)
        lines = jnp.sum(dots_recv[e, :, :count], axis=0)
        total = jnp.sum(lines, axis=1, keepdims=True)
        return [jnp.broadcast_to(total[j : j + 1], (1, width)) for j in range(count)]

    def fold(product):
        return jnp.sum(product.reshape(width // SUBLANES, SUBLANES, width), axis=0)

    def send_products(e, value, products=()):
        if e > 0:
            vec[e] = value
        if products:
            dots_start(e - 1, products)

        def some_rows(g, carry):
            if e == 0:
                for load in piece_loads(g):
                    load.wait()
            for u in range(unroll):
                r = g * unroll + u
                line = vec[e, pl.ds(r, 1)] if e > 0 else right_ref[pl.ds(r, 1)]
                hat = jnp.sum(jac[r] * line, axis=1, keepdims=True)
                hat = jnp.broadcast_to(hat, (width, width))
                for k in range(slot_count):
                    at = pl.multiple_of(k * chunk + r * SUBLANES, SUBLANES)
                    prod[pl.ds(at, SUBLANES)] = fold(coup[r, k] * hat)
                dprod[pl.ds(pl.multiple_of(r * SUBLANES, SUBLANES), SUBLANES)] = fold(diag[r] * hat)
            return carry

        lax.fori_loop(0, rows_dev // unroll, some_rows, 0)
        rest = prod[...]
        out = None
        for _ in range(2):
            piece = rest.astype(jnp.bfloat16)
            rest = rest - piece.astype(F32)
            term = jnp.dot(one_hot[...], piece, preferred_element_type=F32)
            out = term if out is None else out + term
        landed[e] = out
        if e == last:
            at = pl.multiple_of(sub * rows_dev, rows_dev)
            own = jnp.sum(dprod[...].reshape(rows_dev, SUBLANES, width), axis=1)
            own = jnp.where(col == 0, own, 0.0)
            landed[e, pl.ds(at, rows_dev)] = landed[e, pl.ds(at, rows_dev)] + own
            for slot in far_first:
                for across in reversed(range(n_cols)):
                    send = functools.partial(lambda s, a: hub_copy(s, a).start(), slot, across)
                    if (slot, across) == (0, 0):
                        off_hub(send)
                    else:
                        if_linked(slot, send)
            return
        if e == 0:
            greetings = peers - 1 + (n_cols - 1) * n_sub * linked_count
            pl.semaphore_wait(barrier, greetings)
        each_route(lambda slot, step: owner_copy(e, slot, step).start())

    def own_products(e):
        at = pl.multiple_of(from_block(0, col, sub), rows_dev)
        from_at = pl.multiple_of(sub * rows_dev, rows_dev)
        recv[e, pl.ds(at, rows_dev)] = landed[e, pl.ds(from_at, rows_dev)]
        return jnp.sum(dprod[...].reshape(rows_dev, SUBLANES, width), axis=1)

    def gather_products(e, own):
        await_blocks(recv_sem.at[e])
        for b in range(slots * n_cols * n_sub):
            own = own + recv[e, b * rows_dev : (b + 1) * rows_dev]
        return own

    shadow = right_ref[...]
    send_products(0, shadow)
    own = own_products(0)
    image = gather_products(0, own)

    send_products(1, image, [shadow * shadow, shadow * image])
    own = own_products(1)
    rho, shadow_image = dots_finish(0, 2)
    alpha = rho / shadow_image
    half = shadow - alpha * image
    second = gather_products(1, own)
    twice = image - alpha * second

    send_products(2, twice, [twice * half, twice * twice, shadow * half, shadow * twice])
    own = own_products(2)
    cross, square, shadow_half, shadow_twice = dots_finish(1, 4)
    omega = cross / square
    rho_next = shadow_half - omega * shadow_twice
    beta = rho_next / rho * (alpha / omega)
    residual = half - omega * twice
    search = residual + beta * (shadow - omega * image)
    known = twice + beta * (image - omega * second)
    third = gather_products(2, own)
    residual_image = twice - omega * third
    image = known - omega * third
    kept[sub, 0] = residual_image
    kept[sub, 1] = residual
    kept[sub, 2] = image

    @off_hub
    def _():
        core_copy(kept, sub, hub, 0).start()

    send_products(3, image, [shadow * image])
    alpha_next = rho_next / dots_finish(2, 1)[0]
    half_next = residual - alpha_next * image

    @at_hub
    def _():
        at = pl.multiple_of(from_block(0, col, sub) * n_sub, part_rows)
        hub_recv[pl.ds(at, part_rows)] = landed[last, :part_rows]
        if n_sub > 1:
            await_rows(core_sem.at[1], (n_sub - 1) * 3 * rows_dev)
        for_linked_count(
            lambda total: await_rows(recv_sem.at[last], (total * n_cols * n_sub - 1) * part_rows)
        )
        fourth = hub_recv[:part_rows]
        for b in range(1, slots * n_cols * n_sub):
            fourth = fourth + hub_recv[b * part_rows : (b + 1) * part_rows]
        cross = jnp.zeros((rows_dev, width), F32)
        square = jnp.zeros((rows_dev, width), F32)
        for t in range(n_sub):
            end = kept[t, 0] - alpha_next * fourth[t * rows_dev : (t + 1) * rows_dev]
            cross = cross + end * (kept[t, 1] - alpha_next * kept[t, 2])
            square = square + end * end
            ends[t] = end
        for j, product in enumerate((cross, square)):
            dots[last, j : j + 1] = jnp.sum(product, axis=0, keepdims=True)
        for _, where in dot_peers():
            dots_copy(last, 2, where).start()
        for t in range(hub):
            core_copy(ends, t, t, 1).start()
        dots_recv[last, me, :2] = dots[last, :2]

    vec[0] = alpha * shadow + omega * half + alpha_next * search
    vec[1] = half_next
    at_lane = lax.broadcasted_iota(jnp.int32, (width, width), 1)

    def hats(r, carry):
        for j in range(2):
            hat = jnp.sum(jac[r] * vec[j, pl.ds(r, 1)], axis=1, keepdims=True)
            carry = jnp.where(at_lane == j * rows_dev + r, hat, carry)
        return carry

    hat = lax.fori_loop(0, rows_dev, hats, jnp.zeros((width, width), F32), unroll=4)
    hat = jnp.transpose(hat)
    for e in range(last):
        await_blocks(send_sem.at[e])
    for e, count in enumerate((2, 4, 1)):
        await_rows(dots_send_sem.at[e], (peers - 1) * count)

    @at_hub
    def _():
        for_linked_count(
            lambda total: await_rows(send_sem.at[last], (total * n_cols - 1) * part_rows)
        )
        await_rows(dots_send_sem.at[last], (peers - 1) * 2)
        if hub > 0:
            await_rows(core_sem.at[2], hub * rows_dev)
        await_rows(dots_recv_sem.at[last], (n_rows - 1) * 2)

    @off_hub
    def _():
        for_linked_count(lambda total: await_rows(send_sem.at[last], total * n_cols * part_rows))
        await_rows(core_sem.at[0], 3 * rows_dev)
        await_rows(core_sem.at[3], rows_dev)
        await_rows(dots_recv_sem.at[last], n_rows * 2)

    lines = dots_recv[last, hub, :2]
    for r in range(1, n_rows):
        lines = lines + dots_recv[last, r * n_sub + hub, :2]
    total = jnp.sum(lines, axis=1, keepdims=True)
    omega = jnp.broadcast_to(total[:1], (1, width)) / jnp.broadcast_to(total[1:], (1, width))
    out_ref[:rows_dev] = hat[:rows_dev] + omega * hat[rows_dev : 2 * rows_dev]
    out_ref[rows_dev:] = half_next - omega * ends[sub]


def on_device(
    diagonal_tiles, coupling_tiles, column_part, column_tile, neighbours, right_side, jacobi_inverse
):
    n_rows, n_cols, n_sub = (lax.axis_size(a) for a in ("rows", "cols", "sub"))
    slots = len(offsets_of(n_rows))
    rows_dev, slot_count, width, _ = coupling_tiles.shape
    part_rows = n_sub * rows_dev
    chunk = rows_dev * SUBLANES
    peers = n_rows * n_sub
    hbm = pl.BlockSpec(memory_space=pl.ANY)
    vmem = pl.BlockSpec(memory_space=pltpu.VMEM)
    dma = pltpu.SemaphoreType.DMA
    scratch = [
        pltpu.VMEM(diagonal_tiles.shape, F32),
        pltpu.VMEM(coupling_tiles.shape, F32),
        pltpu.VMEM(jacobi_inverse.shape, F32),
        pltpu.VMEM((slot_count, rows_dev), jnp.int32),
        pltpu.VMEM((slot_count, rows_dev), jnp.int32),
        pltpu.SMEM(neighbours.shape, jnp.int32),
        pltpu.VMEM(right_side.shape, F32),
        pltpu.VMEM((slots * part_rows, slot_count * chunk), jnp.bfloat16),
        pltpu.VMEM((slot_count * chunk, width), F32),
        pltpu.VMEM((chunk, width), F32),
        pltpu.VMEM((APPLIES, rows_dev, width), F32),
        pltpu.VMEM((APPLIES, slots * part_rows, width), F32),
        pltpu.VMEM((APPLIES - 1, slots * n_cols * part_rows, width), F32),
        pltpu.VMEM((slots * n_cols * n_sub * part_rows, width), F32),
        pltpu.VMEM((n_sub, 3, rows_dev, width), F32),
        pltpu.VMEM((n_sub, rows_dev, width), F32),
        pltpu.VMEM((APPLIES, SUBLANES, width), F32),
        pltpu.VMEM((APPLIES, peers, SUBLANES, width), F32),
        dma((5 + 2 * (rows_dev // pieces_of(rows_dev)),)),
        dma((APPLIES,)),
        dma((APPLIES,)),
        dma((APPLIES,)),
        dma((APPLIES,)),
        dma((4,)),
    ]
    both = pl.pallas_call(
        functools.partial(kernel, (n_rows, n_cols, n_sub)),
        out_shape=pltpu.VMEM((2 * rows_dev, width), F32),
        in_specs=[hbm] * 7,
        out_specs=vmem,
        scratch_shapes=scratch,
        compiler_params=pltpu.CompilerParams(
            collective_id=0, has_side_effects=True, vmem_limit_bytes=56 * 2**20
        ),
        name="solve",
    )(
        diagonal_tiles,
        coupling_tiles,
        jacobi_inverse,
        column_part.T,
        column_tile.T,
        neighbours,
        right_side,
    )
    return both[:rows_dev], both[rows_dev:]


def solution(mesh):
    in_specs = (
        P(("groups", "rows", "sub"), None, None),
        P(("groups", "rows", "sub"), "cols", None, None),
        P(("groups", "rows", "sub"), "cols"),
        P(("groups", "rows", "sub"), "cols"),
        P("groups", None),
        P(("groups", "rows", "sub"), None),
        P(("groups", "rows", "sub"), None, None),
    )
    out_specs = (P(("groups", "rows", "sub"), None), P(("groups", "rows", "sub"), None))
    return jax.shard_map(
        on_device, mesh=mesh, in_specs=in_specs, out_specs=out_specs, check_vma=False
    )
```

```python
import functools

import jax
import jax.numpy as jnp
from jax import lax
from jax.experimental import pallas as pl
from jax.experimental.pallas import tpu as pltpu
from jax.sharding import PartitionSpec as P

MESH = pl.DeviceIdType.MESH
REACH = 2
APPLIES = 4
SUBLANES = 8
MOST_DOTS = 4
F32 = jnp.float32


def offsets_of(count):
    wanted = {d % count for d in range(-REACH, REACH + 1)} | {count // 2}
    return sorted(wanted)


def pieces_of(rows):
    return 8 if rows % 8 == 0 else 1


def kernel(
    sizes,
    diag_hbm,
    coup_hbm,
    jac_hbm,
    part_hbm,
    tile_hbm,
    near_hbm,
    right_hbm,
    out_ref,
    diag,
    coup,
    jac,
    part_ref,
    tile_ref,
    near_ref,
    right_ref,
    one_hot,
    prod,
    dprod,
    vec,
    landed,
    recv,
    hub_recv,
    kept,
    ends,
    dots,
    dots_recv,
    load_sem,
    send_sem,
    recv_sem,
    dots_send_sem,
    dots_recv_sem,
    core_sem,
):
    n_rows, n_cols, n_sub = sizes
    offsets = offsets_of(n_rows)
    slots = len(offsets)
    rows_dev, slot_count, width, _ = coup.shape
    part_rows = n_sub * rows_dev
    chunk = rows_dev * SUBLANES
    peers = n_rows * n_sub
    hub = n_sub - 1
    last = APPLIES - 1
    unroll = pieces_of(rows_dev)
    row = lax.axis_index("rows")
    col = lax.axis_index("cols")
    sub = lax.axis_index("sub")
    me = row * n_sub + sub

    def piece_loads(g):
        at = pl.ds(g * unroll, unroll)
        first_sem = 5 + (1 + slot_count) * g
        loads = [pltpu.make_async_copy(diag_hbm.at[at], diag.at[at], load_sem.at[first_sem])]
        for k in range(slot_count):
            sem = load_sem.at[first_sem + 1 + k]
            loads.append(pltpu.make_async_copy(coup_hbm.at[at, k], coup.at[at, k], sem))
        return loads

    small = [
        pltpu.make_async_copy(part_hbm, part_ref, load_sem.at[0]),
        pltpu.make_async_copy(tile_hbm, tile_ref, load_sem.at[1]),
        pltpu.make_async_copy(near_hbm, near_ref, load_sem.at[2]),
        pltpu.make_async_copy(right_hbm, right_ref, load_sem.at[3]),
    ]
    jac_load = pltpu.make_async_copy(jac_hbm, jac, load_sem.at[4])
    for load in small:
        load.start()
    jac_load.start()
    for g in range(rows_dev // unroll):
        for load in piece_loads(g):
            load.start()

    def partner(slot):
        return lax.rem(row + offsets[slot], n_rows)

    def always(slot):
        return offsets[slot] in (0, n_rows // 2)

    def is_linked(slot):
        return jnp.abs(partner(slot) - row) <= REACH

    def if_linked(slot, act):
        if always(slot):
            act()
        else:
            pl.when(is_linked(slot))(act)

    maybe = [slot for slot in range(slots) if not always(slot)]
    linked_count = slots - len(maybe)
    for slot in maybe:
        linked_count = linked_count + is_linked(slot).astype(jnp.int32)

    def for_linked_count(act):
        if not maybe:
            act(slots)
        for total in range(slots - len(maybe), slots + 1) if maybe else ():
            pl.when(linked_count == total)(functools.partial(act, total))

    def corner(slot, step):
        return {
            "rows": partner(slot),
            "cols": lax.rem(col + step // n_sub, n_cols),
            "sub": lax.rem(sub + step % n_sub, n_sub),
        }

    barrier = pltpu.get_barrier_semaphore()

    def dot_peers():
        for step in range(1, peers):
            peer = lax.rem(me + step, peers)
            yield peer, {"rows": lax.div(peer, n_sub), "cols": col, "sub": lax.rem(peer, n_sub)}

    def from_block(slot, c, s):
        return ((slot * n_cols + c) * n_sub + s) * rows_dev

    per_slot = n_cols * n_sub * rows_dev
    for slot in maybe:
        at = pl.ds(slot * per_slot, per_slot)
        for e in range(last):
            recv[e, at] = jnp.zeros((per_slot, width), F32)
        hub_recv[slot * per_slot * n_sub : (slot + 1) * per_slot * n_sub] = jnp.zeros(
            (per_slot * n_sub, width), F32
        )

    far_first = sorted(range(slots), key=lambda s: -min(offsets[s], n_rows - offsets[s]))
    for slot in far_first:
        for step in range(n_sub, n_cols * n_sub):

            def greet(slot=slot, step=step):
                where = corner(slot, step)
                pl.semaphore_signal(barrier, inc=1, device_id=where, device_id_type=MESH)

            if_linked(slot, greet)
    for _, where in dot_peers():
        pl.semaphore_signal(barrier, inc=1, device_id=where, device_id_type=MESH)

    for load in small:
        load.wait()
    part = part_ref[...]
    tile = tile_ref[...]
    target = jnp.full(part.shape, row, jnp.int32)
    for j in range(near_ref.shape[1]):
        target = jnp.where(part == j + 1, near_ref[row, j], target)
    apart = target - row
    apart = jnp.where(apart < 0, apart + n_rows, apart)
    place = jnp.zeros(part.shape, jnp.int32)
    for slot in range(1, slots):
        place = jnp.where(apart == offsets[slot], slot, place)
    landing = place * part_rows + tile
    from_row = lax.broadcasted_iota(jnp.int32, (rows_dev, chunk), 0)
    to_lane = lax.broadcasted_iota(jnp.int32, (rows_dev, chunk), 1)
    first = from_row * SUBLANES
    spread = ((to_lane >= first) & (to_lane < first + SUBLANES)).astype(F32)
    spread_landing = jnp.dot(
        landing.astype(F32), spread, precision=lax.Precision.HIGHEST, preferred_element_type=F32
    )
    at_row = lax.broadcasted_iota(jnp.int32, (slots * part_rows, chunk), 0).astype(F32)
    for k in range(slot_count):
        hit = (spread_landing[k : k + 1] == at_row).astype(F32)
        one_hot[:, k * chunk : (k + 1) * chunk] = hit.astype(jnp.bfloat16)

    jac_load.wait()

    def turn(r, carry):
        jac[r] = jnp.transpose(jac[r])
        return carry

    lax.fori_loop(0, rows_dev, turn, 0, unroll=4)

    def owner_copy(e, slot, step):
        back = offsets.index(-offsets[slot] % n_rows)
        where = corner(slot, step)
        at = pl.multiple_of(slot * part_rows + where["sub"] * rows_dev, rows_dev)
        to = pl.multiple_of(from_block(back, col, sub), rows_dev)
        return pltpu.make_async_remote_copy(
            src_ref=landed.at[e, pl.ds(at, rows_dev)],
            dst_ref=recv.at[e, pl.ds(to, rows_dev)],
            send_sem=send_sem.at[e],
            recv_sem=recv_sem.at[e],
            device_id=where,
            device_id_type=MESH,
        )

    routes = [(s, c) for s in far_first for c in reversed(range(n_cols * n_sub)) if (s, c) != (0, 0)]

    def each_route(act):
        for slot, step in routes:
            if_linked(slot, functools.partial(act, slot, step))

    def hub_copy(slot, across):
        back = offsets.index(-offsets[slot] % n_rows)
        to = pl.multiple_of(from_block(back, col, sub) * n_sub, part_rows)
        return pltpu.make_async_remote_copy(
            src_ref=landed.at[last, pl.ds(slot * part_rows, part_rows)],
            dst_ref=hub_recv.at[pl.ds(to, part_rows)],
            send_sem=send_sem.at[last],
            recv_sem=recv_sem.at[last],
            device_id={
                "rows": partner(slot),
                "cols": lax.rem(col + across, n_cols),
                "sub": jnp.int32(hub),
            },
            device_id_type=MESH,
        )

    def core_copy(ref, index, to, which):
        return pltpu.make_async_remote_copy(
            src_ref=ref.at[index],
            dst_ref=ref.at[index],
            send_sem=core_sem.at[2 * which],
            recv_sem=core_sem.at[2 * which + 1],
            device_id={"rows": row, "cols": col, "sub": jnp.int32(to)},
            device_id_type=MESH,
        )

    def at_hub(act):
        pl.when(sub == hub)(act)

    def off_hub(act):
        pl.when(sub != hub)(act)

    def await_rows(sem, count):
        some = hub_recv.at[pl.ds(0, count)]
        pltpu.make_async_copy(some, some, sem).wait()

    def await_blocks(sem):
        for_linked_count(lambda total: await_rows(sem, total * per_slot - rows_dev))

    def dots_copy(e, count, where):
        return pltpu.make_async_remote_copy(
            src_ref=dots.at[e, pl.ds(0, count)],
            dst_ref=dots_recv.at[e, me, pl.ds(0, count)],
            send_sem=dots_send_sem.at[e],
            recv_sem=dots_recv_sem.at[e],
            device_id=where,
            device_id_type=MESH,
        )

    def dots_start(e, products):
        count = len(products)
        lines = [jnp.sum(product, axis=0, keepdims=True) for product in products]
        for j, line in enumerate(lines):
            dots[e, j : j + 1] = line
        for _, where in dot_peers():
            dots_copy(e, count, where).start()
        for j, line in enumerate(lines):
            dots_recv[e, me, j : j + 1] = line

    def dots_finish(e, count):
        await_rows(dots_recv_sem.at[e], (peers - 1) * count)
        lines = jnp.sum(dots_recv[e, :, :count], axis=0)
        total = jnp.sum(lines, axis=1, keepdims=True)
        return [jnp.broadcast_to(total[j : j + 1], (1, width)) for j in range(count)]

    def fold(product):
        return jnp.sum(product.reshape(width // SUBLANES, SUBLANES, width), axis=0)

    def send_products(e, value, products=()):
        if e > 0:
            vec[e] = value
        if products:
            dots_start(e - 1, products)

        def some_rows(g, carry):
            if e == 0:
                for load in piece_loads(g):
                    load.wait()
            for u in range(unroll):
                r = g * unroll + u
                line = vec[e, pl.ds(r, 1)] if e > 0 else right_ref[pl.ds(r, 1)]
                hat = jnp.sum(jac[r] * line, axis=1, keepdims=True)
                hat = jnp.broadcast_to(hat, (width, width))
                for k in range(slot_count):
                    at = pl.multiple_of(k * chunk + r * SUBLANES, SUBLANES)
                    prod[pl.ds(at, SUBLANES)] = fold(coup[r, k] * hat)
                dprod[pl.ds(pl.multiple_of(r * SUBLANES, SUBLANES), SUBLANES)] = fold(diag[r] * hat)
            return carry

        lax.fori_loop(0, rows_dev // unroll, some_rows, 0)
        rest = prod[...]
        out = None
        for _ in range(2):
            piece = rest.astype(jnp.bfloat16)
            rest = rest - piece.astype(F32)
            term = jnp.dot(one_hot[...], piece, preferred_element_type=F32)
            out = term if out is None else out + term
        landed[e] = out
        if e == last:
            at = pl.multiple_of(sub * rows_dev, rows_dev)
            own = jnp.sum(dprod[...].reshape(rows_dev, SUBLANES, width), axis=1)
            own = jnp.where(col == 0, own, 0.0)
            landed[e, pl.ds(at, rows_dev)] = landed[e, pl.ds(at, rows_dev)] + own
            for slot in far_first:
                for across in reversed(range(n_cols)):
                    send = functools.partial(lambda s, a: hub_copy(s, a).start(), slot, across)
                    if (slot, across) == (0, 0):
                        off_hub(send)
                    else:
                        if_linked(slot, send)
            return
        if e == 0:
            greetings = peers - 1 + (n_cols - 1) * n_sub * linked_count
            pl.semaphore_wait(barrier, greetings)
        each_route(lambda slot, step: owner_copy(e, slot, step).start())

    def own_products(e):
        at = pl.multiple_of(from_block(0, col, sub), rows_dev)
        from_at = pl.multiple_of(sub * rows_dev, rows_dev)
        recv[e, pl.ds(at, rows_dev)] = landed[e, pl.ds(from_at, rows_dev)]
        return jnp.sum(dprod[...].reshape(rows_dev, SUBLANES, width), axis=1)

    def gather_products(e, own):
        await_blocks(recv_sem.at[e])
        for b in range(slots * n_cols * n_sub):
            own = own + recv[e, b * rows_dev : (b + 1) * rows_dev]
        return own

    shadow = right_ref[...]
    send_products(0, shadow)
    own = own_products(0)
    image = gather_products(0, own)

    send_products(1, image, [shadow * shadow, shadow * image])
    own = own_products(1)
    rho, shadow_image = dots_finish(0, 2)
    alpha = rho / shadow_image
    half = shadow - alpha * image
    second = gather_products(1, own)
    twice = image - alpha * second

    send_products(2, twice, [twice * half, twice * twice, shadow * half, shadow * twice])
    own = own_products(2)
    cross, square, shadow_half, shadow_twice = dots_finish(1, 4)
    omega = cross / square
    rho_next = shadow_half - omega * shadow_twice
    beta = rho_next / rho * (alpha / omega)
    residual = half - omega * twice
    search = residual + beta * (shadow - omega * image)
    known = twice + beta * (image - omega * second)
    third = gather_products(2, own)
    residual_image = twice - omega * third
    image = known - omega * third
    kept[sub, 0] = residual_image
    kept[sub, 1] = residual
    kept[sub, 2] = image

    @off_hub
    def _():
        core_copy(kept, sub, hub, 0).start()

    send_products(3, image, [shadow * image])
    alpha_next = rho_next / dots_finish(2, 1)[0]
    half_next = residual - alpha_next * image

    @at_hub
    def _():
        at = pl.multiple_of(from_block(0, col, sub) * n_sub, part_rows)
        hub_recv[pl.ds(at, part_rows)] = landed[last, :part_rows]
        if n_sub > 1:
            await_rows(core_sem.at[1], (n_sub - 1) * 3 * rows_dev)
        for_linked_count(
            lambda total: await_rows(recv_sem.at[last], (total * n_cols * n_sub - 1) * part_rows)
        )
        fourth = hub_recv[:part_rows]
        for b in range(1, slots * n_cols * n_sub):
            fourth = fourth + hub_recv[b * part_rows : (b + 1) * part_rows]
        cross = jnp.zeros((rows_dev, width), F32)
        square = jnp.zeros((rows_dev, width), F32)
        for t in range(n_sub):
            end = kept[t, 0] - alpha_next * fourth[t * rows_dev : (t + 1) * rows_dev]
            cross = cross + end * (kept[t, 1] - alpha_next * kept[t, 2])
            square = square + end * end
            ends[t] = end
        for j, product in enumerate((cross, square)):
            dots[last, j : j + 1] = jnp.sum(product, axis=0, keepdims=True)
        for _, where in dot_peers():
            dots_copy(last, 2, where).start()
        for t in range(hub):
            core_copy(ends, t, t, 1).start()
        dots_recv[last, me, :2] = dots[last, :2]

    vec[0] = alpha * shadow + omega * half + alpha_next * search
    vec[1] = half_next
    at_lane = lax.broadcasted_iota(jnp.int32, (width, width), 1)

    def hats(r, carry):
        for j in range(2):
            hat = jnp.sum(jac[r] * vec[j, pl.ds(r, 1)], axis=1, keepdims=True)
            carry = jnp.where(at_lane == j * rows_dev + r, hat, carry)
        return carry

    hat = lax.fori_loop(0, rows_dev, hats, jnp.zeros((width, width), F32), unroll=4)
    hat = jnp.transpose(hat)
    for e in range(last):
        await_blocks(send_sem.at[e])
    for e, count in enumerate((2, 4, 1)):
        await_rows(dots_send_sem.at[e], (peers - 1) * count)

    @at_hub
    def _():
        for_linked_count(
            lambda total: await_rows(send_sem.at[last], (total * n_cols - 1) * part_rows)
        )
        await_rows(dots_send_sem.at[last], (peers - 1) * 2)
        if hub > 0:
            await_rows(core_sem.at[2], hub * rows_dev)
        await_rows(dots_recv_sem.at[last], (n_rows - 1) * 2)

    @off_hub
    def _():
        for_linked_count(lambda total: await_rows(send_sem.at[last], total * n_cols * part_rows))
        await_rows(core_sem.at[0], 3 * rows_dev)
        await_rows(core_sem.at[3], rows_dev)
        await_rows(dots_recv_sem.at[last], n_rows * 2)

    lines = dots_recv[last, hub, :2]
    for r in range(1, n_rows):
        lines = lines + dots_recv[last, r * n_sub + hub, :2]
    total = jnp.sum(lines, axis=1, keepdims=True)
    omega = jnp.broadcast_to(total[:1], (1, width)) / jnp.broadcast_to(total[1:], (1, width))
    out_ref[:rows_dev] = hat[:rows_dev] + omega * hat[rows_dev : 2 * rows_dev]
    out_ref[rows_dev:] = half_next - omega * ends[sub]


def on_device(
    diagonal_tiles, coupling_tiles, column_part, column_tile, neighbours, right_side, jacobi_inverse
):
    n_rows, n_cols, n_sub = (lax.axis_size(a) for a in ("rows", "cols", "sub"))
    slots = len(offsets_of(n_rows))
    rows_dev, slot_count, width, _ = coupling_tiles.shape
    part_rows = n_sub * rows_dev
    chunk = rows_dev * SUBLANES
    peers = n_rows * n_sub
    hbm = pl.BlockSpec(memory_space=pl.ANY)
    vmem = pl.BlockSpec(memory_space=pltpu.VMEM)
    dma = pltpu.SemaphoreType.DMA
    scratch = [
        pltpu.VMEM(diagonal_tiles.shape, F32),
        pltpu.VMEM(coupling_tiles.shape, F32),
        pltpu.VMEM(jacobi_inverse.shape, F32),
        pltpu.VMEM((slot_count, rows_dev), jnp.int32),
        pltpu.VMEM((slot_count, rows_dev), jnp.int32),
        pltpu.SMEM(neighbours.shape, jnp.int32),
        pltpu.VMEM(right_side.shape, F32),
        pltpu.VMEM((slots * part_rows, slot_count * chunk), jnp.bfloat16),
        pltpu.VMEM((slot_count * chunk, width), F32),
        pltpu.VMEM((chunk, width), F32),
        pltpu.VMEM((APPLIES, rows_dev, width), F32),
        pltpu.VMEM((APPLIES, slots * part_rows, width), F32),
        pltpu.VMEM((APPLIES - 1, slots * n_cols * part_rows, width), F32),
        pltpu.VMEM((slots * n_cols * n_sub * part_rows, width), F32),
        pltpu.VMEM((n_sub, 3, rows_dev, width), F32),
        pltpu.VMEM((n_sub, rows_dev, width), F32),
        pltpu.VMEM((APPLIES, SUBLANES, width), F32),
        pltpu.VMEM((APPLIES, peers, SUBLANES, width), F32),
        dma((5 + (1 + slot_count) * (rows_dev // pieces_of(rows_dev)),)),
        dma((APPLIES,)),
        dma((APPLIES,)),
        dma((APPLIES,)),
        dma((APPLIES,)),
        dma((4,)),
    ]
    both = pl.pallas_call(
        functools.partial(kernel, (n_rows, n_cols, n_sub)),
        out_shape=pltpu.VMEM((2 * rows_dev, width), F32),
        in_specs=[hbm] * 7,
        out_specs=vmem,
        scratch_shapes=scratch,
        compiler_params=pltpu.CompilerParams(
            collective_id=0, has_side_effects=True, vmem_limit_bytes=56 * 2**20
        ),
        name="solve",
    )(
        diagonal_tiles,
        coupling_tiles,
        jacobi_inverse,
        column_part.T,
        column_tile.T,
        neighbours,
        right_side,
    )
    return both[:rows_dev], both[rows_dev:]


def solution(mesh):
    in_specs = (
        P(("groups", "rows", "sub"), None, None),
        P(("groups", "rows", "sub"), "cols", None, None),
        P(("groups", "rows", "sub"), "cols"),
        P(("groups", "rows", "sub"), "cols"),
        P("groups", None),
        P(("groups", "rows", "sub"), None),
        P(("groups", "rows", "sub"), None, None),
    )
    out_specs = (P(("groups", "rows", "sub"), None), P(("groups", "rows", "sub"), None))
    return jax.shard_map(
        on_device, mesh=mesh, in_specs=in_specs, out_specs=out_specs, check_vma=False
    )
```
